128 devices in a mesh: dp: 8 (over y_hi, z), mp: 16 (over y_lo, x, core).
Axes of the slice: x: 4, y: 4 (y_hi: 2, y_lo: 2; y = y_hi * 2 + y_lo), z: 4, core: 2. Of those that a mesh axis runs over, the one named last changes fastest.
Arguments:
- weight: bfloat16 [5120, 32768], P('dp', 'mp'), may hold values from -0.078125 to 0.078125
- rank_map: int32 [16], replicated, may hold values from 0 to 15, each once
Outputs:
- quant_out: bfloat16 [5120, 32768], P(None, 'mp')
- scale_out: bfloat16 [5120, 256], P(None, 'mp')
- checksum: float32 [256], replicated
The draws below stay inside these ranges and needn't reach their ends.
Inputs may be any that keep to these rules, and one draw needn't show every extreme that they name: `rank_map`: a permutation of 0 to 15.
All inputs are finite; a program needn't handle non-finite values.
Results may differ from the reference program's by a relative error of at most 0.0085.
Values may be sent and summed in bfloat16 or wider, within the bound.
A program may use at most 192 MiB of HBM per device.

```python
import math
import jax
import jax.numpy as jnp
from jax import lax

D = 5120
F = 32768
N_MP = 16


def level_of(key, shape, pieces, smallest, largest):
    factor_of = 1.0
    for position, parts in pieces:
        draws = jax.random.uniform(jax.random.fold_in(jax.random.fold_in(key, 6), position), (parts,), jnp.float32, smallest / len(pieces), largest / len(pieces))
        factor_of = factor_of * jnp.repeat(jnp.exp(draws), shape[position] // parts).reshape((-1,) + (1,) * (len(shape) - 1 - position))
    return factor_of


def scatter_about(stream_key, dims, deviation, limit, shards=(), dtype=jnp.bfloat16):
    values = jax.random.normal(stream_key, dims, jnp.float32) * deviation
    if len(shards) > 0:
        values = level_of(stream_key, dims, shards, -0.22, 0.18) * values
    return jnp.clip(values, min=-limit, max=limit).astype(dtype)


def setup_inputs(seed: int = 0) -> dict:
    key_of = jax.random.split(jax.random.key(seed), 3)
    weight = scatter_about(key_of[0], (D, F), D ** -0.5, 0.078125, ((0, 8), (1, 16)))
    rank_map = jax.random.permutation(key_of[1], N_MP).astype(jnp.int32)
    return {"weight": weight, "rank_map": rank_map}


floor_ratio = 0.25

def quantize(weight):
    rows, cols = weight.shape
    blocks = weight.astype(jnp.float32).reshape(rows, cols // 128, 128)
    peak = lax.optimization_barrier(jnp.max(jnp.abs(blocks), axis=2))
    scale = (jnp.maximum(peak, floor_ratio / math.sqrt(D)) / 127.0).astype(jnp.bfloat16)
    quant = (blocks / scale.astype(jnp.float32)[:, :, None]).astype(jnp.bfloat16)
    return (quant, scale)

def inverse(rank_map):
    count = rank_map.shape[0]
    ids = jnp.arange(count).astype(jnp.int32)
    match = (rank_map[None, :] == ids[:, None]).astype(jnp.int32)
    return lax.optimization_barrier(jnp.sum(ids[None, :] * match, axis=1)).astype(jnp.int32)

def reference(weight, rank_map):
    quant, scale = quantize(weight)
    total = lax.optimization_barrier(jnp.sum(quant.astype(jnp.float32), axis=(0, 2)))
    checksum = total / (127.0 * math.sqrt(D * 128))
    inv = inverse(rank_map)
    blocks = F // 128
    local = blocks // N_MP
    order = (jnp.arange(local).astype(jnp.int32)[None, :] * N_MP + inv[:, None]).reshape(-1).astype(jnp.int32)
    quant_out = jnp.take(quant, order, axis=1).reshape(D, F)
    scale_out = jnp.take(scale, order, axis=1)
    return (quant_out, scale_out, checksum)
```

```python
import functools
import math

import jax
import jax.numpy as jnp
from jax import lax
from jax.experimental import pallas as pl
from jax.experimental.pallas import tpu as pltpu
from jax.sharding import PartitionSpec as P

MESH = pl.DeviceIdType.MESH
D = 5120
floor_ratio = 0.25
BLOCK = 128
ROWS = 640
PIECE = 656
N_MP = 16
N_DP = 8
GROUPS = 8
Z = 4
MIB = 1024 * 1024


def exchange(rank_ref, w_hbm, land, sums, w, staged, part, parts, w_sem, recv1, recvz, send, sem_a, sem_b, send_s):
    dp = lax.axis_index("dp")
    mp = lax.axis_index("mp")
    h, z = dp // Z, lax.rem(dp, Z)
    yl, x, c = mp // 8, lax.rem(mp // 2, 4), lax.rem(mp, 2)

    for q in range(N_MP):
        pltpu.make_async_copy(w_hbm.at[:, pl.ds(q * BLOCK, BLOCK)], w.at[q], w_sem).start()

    def z_at(dz):
        return lax.rem(z + dz, Z)

    def rank_at(yy, xx, cc):
        return yy * 8 + xx * 2 + cc

    def target(u, cc):
        return rank_at(lax.rem(yl + lax.rem(u, 2), 2), lax.rem(x + u // 2, 4), lax.rem(c + cc, 2))

    def origin(u, cs):
        return rank_at(lax.rem(yl + lax.rem(u, 2), 2), lax.rem(x + 4 - u // 2, 4), cs)

    barrier = pltpu.get_barrier_semaphore()

    def greet(n, _):
        hh, r = n // N_MP, lax.rem(mp + lax.rem(n, N_MP), N_MP)
        pl.semaphore_signal(barrier, inc=1, device_id=(lax.rem(h + hh, 2) * Z + z, r), device_id_type=MESH)
        return 0

    lax.fori_loop(1, 2 * N_MP, greet, 0)
    for dz in (1, 2, 3):
        for hh in (0, 1):
            pl.semaphore_signal(barrier, inc=1, device_id=(lax.rem(h + hh, 2) * Z + z_at(dz), mp), device_id_type=MESH)

    rows_i = lax.broadcasted_iota(jnp.int32, (BLOCK, BLOCK), 0)
    cols_i = lax.broadcasted_iota(jnp.int32, (BLOCK, BLOCK), 1)
    diag = rows_i == cols_i

    def quantize(r):
        j = jnp.int32(0)
        for q in range(N_MP):
            j = j + jnp.where(rank_ref[q] == r, jnp.int32(q), jnp.int32(0))
        j = jnp.minimum(j, N_MP - 1)
        acc = jnp.zeros((8, BLOCK), jnp.float32)
        scales = []
        for k in range(ROWS // BLOCK):
            blk = w[j, pl.ds(k * BLOCK, BLOCK), :].astype(jnp.float32)
            peak = jnp.max(jnp.abs(blk), axis=1, keepdims=True)
            scale = (jnp.maximum(peak, floor_ratio / math.sqrt(D)) / 127.0).astype(jnp.bfloat16).astype(jnp.float32)
            scale = jnp.broadcast_to(scale, (BLOCK, BLOCK))
            quant = (blk / scale).astype(jnp.bfloat16)
            staged[r, pl.ds(k * BLOCK, BLOCK), :] = quant
            acc = acc + jnp.sum(quant.astype(jnp.float32).reshape(BLOCK // 8, 8, BLOCK), axis=0)
            scales.append(jnp.sum(jnp.where(diag, scale, 0.0), axis=0, keepdims=True))
        scales.append(jnp.zeros((PIECE - ROWS - len(scales), BLOCK), jnp.float32))
        staged[r, pl.ds(ROWS, PIECE - ROWS), :] = jnp.concatenate(scales, axis=0).astype(jnp.bfloat16)
        part[pl.ds(r, 1), :] = jnp.sum(acc, axis=0, keepdims=True)

    def piece_copy(src, dst, sem_s, sem_r, dev):
        return pltpu.make_async_remote_copy(src, dst, sem_s, sem_r, device_id=dev, device_id_type=MESH)

    def first(u, own):
        for cc in (0, 1):
            r = target(u, cc)
            for hh in (0, 1):
                if own and cc == 0 and hh == 0:
                    continue
                dev = (lax.rem(h + hh, 2) * Z + z, r)
                piece_copy(staged.at[r], land.at[dp, mp], send.at[u], recv1.at[u, h * 2 + c], dev).start()

    def step_quant(u, _):
        quantize(target(u, 0))
        quantize(target(u, 1))
        return 0

    def await_recv(sem):
        piece_copy(staged.at[0], staged.at[0], send.at[0], sem, (dp, mp)).wait_recv()

    def spread(u, hs, cs, own=False):
        k = hs * 2 + cs
        if not own:
            await_recv(recv1.at[u, k])
        ref = land.at[hs * Z + z, origin(u, cs)]
        piece_copy(ref, ref, send.at[u], recvz.at[0, u, k], (h * Z + z_at(1), mp)).start()
        piece_copy(ref, ref, send.at[u], recvz.at[1, u, k], (h * Z + z_at(3), mp)).start()

    def onward(u):
        k = h
        await_recv(recvz.at[0, u, k])
        ref = land.at[z_at(3), origin(u, h)]
        piece_copy(ref, ref, send.at[u], recvz.at[2, u, k], (h * Z + z_at(1), mp)).start()
        k = 2 + h
        await_recv(recvz.at[1, u, k])
        ref = land.at[Z + z_at(1), origin(u, h)]
        piece_copy(ref, ref, send.at[u], recvz.at[2, u, k], (h * Z + z_at(3), mp)).start()

    def cross(u):
        for hs in (0, 1):
            k = hs * 2 + h
            await_recv(recvz.at[2, u, k])
            ref = land.at[hs * Z + z_at(2), origin(u, h)]
            piece_copy(ref, ref, send.at[u], recvz.at[2, u, k], ((1 - h) * Z + z, mp)).start()

    def spread_all(u):
        for cs in (h, 1 - h):
            for hs in (0, 1):
                spread(u, hs, cs)

    pltpu.make_async_copy(w, w, w_sem).wait()
    step_quant(0, 0)
    land[dp, mp, :, :] = staged[mp, :, :]
    pl.semaphore_wait(barrier, 2 * N_MP - 1 + 6)
    first(0, True)
    step_quant(1, 0)
    first(1, False)
    for cc in (0, 1):
        for hh in (0, 1):
            spread(0, lax.rem(h + hh, 2), lax.rem(c + cc, 2), own=(cc == 0 and hh == 0))

    def rest(u, _):
        step_quant(u, 0)
        first(u, False)
        return 0

    lax.fori_loop(2, GROUPS, rest, 0)

    parts[dp, :, :] = part[...]
    for hh in (0, 1):
        for dz in range(Z):
            if hh == 0 and dz == 0:
                continue
            dev = (lax.rem(h + hh, 2) * Z + z_at(dz), mp)
            piece_copy(part, parts.at[dp], send_s, sem_a, dev).start()

    spread_all(1)
    onward(0)

    def main(u, _):
        spread_all(u)
        onward(u - 1)
        cross(u - 2)
        return 0

    lax.fori_loop(2, GROUPS, main, 0)

    pltpu.make_async_copy(parts.at[pl.ds(0, 7)], parts.at[pl.ds(0, 7)], sem_a).wait()
    whole = jnp.sum(jnp.sum(parts[...], axis=0), axis=1, keepdims=True)
    sums[mp, :, :] = jnp.broadcast_to(whole, (N_MP, BLOCK))

    onward(GROUPS - 1)

    def share(n, _):
        dev = (dp, lax.rem(mp + n, N_MP))
        piece_copy(sums.at[mp], sums.at[mp], send_s, sem_b, dev).start()
        return 0

    lax.fori_loop(1, N_MP, share, 0)
    cross(GROUPS - 2)
    cross(GROUPS - 1)

    def finish(u, _):
        for k in (1 - h, 2, 3):
            await_recv(recvz.at[0, u, k])
        for k in (0, 1, 3 - h):
            await_recv(recvz.at[1, u, k])
        for k in (1 - h, 3 - h):
            await_recv(recvz.at[2, u, k])
        return 0

    lax.fori_loop(0, GROUPS, finish, 0)
    pltpu.make_async_copy(sums.at[pl.ds(0, 15)], sums.at[pl.ds(0, 15)], sem_b).wait()

    def sent(u, _):
        def one(n, _):
            piece_copy(staged.at[0], staged.at[0], send.at[u], w_sem, (dp, mp)).wait_send()
            return 0

        lax.fori_loop(0, jnp.where(u == 0, 15, 16), one, 0)
        return 0

    lax.fori_loop(0, GROUPS, sent, 0)

    def sent_small(n, _):
        piece_copy(part, part, send_s, w_sem, (dp, mp)).wait_send()
        return 0

    lax.fori_loop(0, 7 + 15, sent_small, 0)


def settle(rank_ref, land, sums, quant_out, scale_out, check_out, sem):
    for d in range(N_DP):
        for i in range(N_MP):
            pltpu.make_async_copy(
                land.at[d, i, pl.ds(0, ROWS), :],
                quant_out.at[pl.ds(d * ROWS, ROWS), pl.ds(i * BLOCK, BLOCK)],
                sem,
            ).start()
    n = PIECE - ROWS
    k_rows = ROWS // BLOCK
    out_i = lax.broadcasted_iota(jnp.int32, (k_rows * N_MP, N_MP * n), 0)
    in_i = lax.broadcasted_iota(jnp.int32, (k_rows * N_MP, N_MP * n), 1)
    pick = (in_i == lax.rem(out_i, N_MP) * n + out_i // N_MP).astype(jnp.bfloat16)
    eye = (
        lax.broadcasted_iota(jnp.int32, (BLOCK, BLOCK), 0) == lax.broadcasted_iota(jnp.int32, (BLOCK, BLOCK), 1)
    ).astype(jnp.bfloat16)

    def scales(d, _):
        rows = land[d, :, pl.ds(ROWS, n), :].reshape(N_MP * n, BLOCK)
        sorted_rows = jnp.dot(pick, rows, preferred_element_type=jnp.float32).astype(jnp.bfloat16)
        for k in range(k_rows):
            flat = lax.dot_general(
                eye, sorted_rows[k * N_MP : (k + 1) * N_MP], (((1,), (1,)), ((), ())), preferred_element_type=jnp.float32
            )
            scale_out[pl.ds(pl.multiple_of(d * ROWS + k * BLOCK, BLOCK), BLOCK), :] = flat.astype(jnp.bfloat16)
        return 0

    lax.fori_loop(0, N_DP, scales, 0)
    lane = lax.broadcasted_iota(jnp.int32, (N_MP, BLOCK), 1)
    total = jnp.zeros((N_MP, BLOCK), jnp.float32)
    for j in range(N_MP):
        total = total + jnp.where(lane == j, sums[:, rank_ref[j], :], 0.0)
    check_out[...] = total / (127.0 * math.sqrt(D * BLOCK))

    def done(n, _):
        pltpu.make_async_copy(
            land.at[0, 0, pl.ds(0, ROWS), :], quant_out.at[pl.ds(0, ROWS), pl.ds(0, BLOCK)], sem
        ).wait()
        return 0

    lax.fori_loop(0, N_DP * N_MP, done, 0)


def local(weight, rank_map):
    vmem = pl.BlockSpec(memory_space=pltpu.VMEM)
    smem = pl.BlockSpec(memory_space=pltpu.SMEM)
    hbm = pl.BlockSpec(memory_space=pl.ANY)
    dma = pltpu.SemaphoreType.DMA
    land, sums = pl.pallas_call(
        exchange,
        out_shape=(
            pltpu.VMEM((N_DP, N_MP, PIECE, BLOCK), jnp.bfloat16),
            pltpu.VMEM((N_MP, N_MP, BLOCK), jnp.float32),
        ),
        in_specs=[smem, pl.BlockSpec(memory_space=pltpu.HBM)],
        out_specs=(vmem, vmem),
        scratch_shapes=[
            pltpu.VMEM((N_MP, ROWS, BLOCK), jnp.bfloat16),
            pltpu.VMEM((N_MP, PIECE, BLOCK), jnp.bfloat16),
            pltpu.VMEM((N_MP, BLOCK), jnp.float32),
            pltpu.VMEM((N_DP, N_MP, BLOCK), jnp.float32),
            dma(()),
            dma((GROUPS, 4)),
            dma((3, GROUPS, 4)),
            dma((GROUPS,)),
            dma(()),
            dma(()),
            dma(()),
        ],
        compiler_params=pltpu.CompilerParams(collective_id=0, has_side_effects=True, vmem_limit_bytes=12 * MIB),
        name="exchange",
    )(rank_map, pltpu.with_memory_space_constraint(weight, pltpu.HBM))
    quant_out, scale_out, check = pl.pallas_call(
        settle,
        out_shape=(
            jax.ShapeDtypeStruct((D, N_MP * BLOCK), jnp.bfloat16),
            jax.ShapeDtypeStruct((D, N_MP), jnp.bfloat16),
            jax.ShapeDtypeStruct((N_MP, BLOCK), jnp.float32),
        ),
        in_specs=[smem, vmem, vmem],
        out_specs=(hbm, vmem, vmem),
        scratch_shapes=[dma(())],
        compiler_params=pltpu.CompilerParams(vmem_limit_bytes=12 * MIB),
        name="settle",
    )(rank_map, land, sums)
    return quant_out, scale_out, check[:, :N_MP].reshape(N_MP * N_MP)


def solution(mesh):
    return jax.shard_map(
        local,
        mesh=mesh,
        in_specs=(P("dp", "mp"), P()),
        out_specs=(P(None, "mp"), P(None, "mp"), P()),
        check_vma=False,
    )
```

```python
import functools
import math

import jax
import jax.numpy as jnp
from jax import lax
from jax.experimental import pallas as pl
from jax.experimental.pallas import tpu as pltpu
from jax.sharding import PartitionSpec as P

MESH = pl.DeviceIdType.MESH
D = 5120
floor_ratio = 0.25
BLOCK = 128
ROWS = 640
PIECE = 656
N_MP = 16
N_DP = 8
STEPS = 8
Z = 4
MIB = 1024 * 1024


def exchange(
    rank_ref, w_hbm, land, sums, w, staged, relay, part, parts, w_sem, recv1, recvr, recvz, send, send_x, sem_a, sem_b, send_s
):
    dp = lax.axis_index("dp")
    mp = lax.axis_index("mp")
    h, z = dp // Z, lax.rem(dp, Z)
    yl, x, c = mp // 8, lax.rem(mp // 2, 4), lax.rem(mp, 2)
    home = yl * 2 + h

    for q in range(N_MP):
        pltpu.make_async_copy(w_hbm.at[:, pl.ds(q * BLOCK, BLOCK)], w.at[q], w_sem).start()

    def z_at(dz):
        return lax.rem(z + dz, Z)

    def rank_at(yy, xx, cc):
        return yy * 8 + xx * 2 + cc

    def shift(m):
        return m + m // 2 - 2 * (m // 3)

    def target(m, yy, cc):
        return rank_at(yy, lax.rem(x + shift(m), 4), cc)

    def origin(s, yy):
        return rank_at(yy, lax.rem(x + 4 - shift(s // 2), 4), lax.rem(c + s, 2))

    barrier = pltpu.get_barrier_semaphore()

    def greet(dev):
        pl.semaphore_signal(barrier, inc=1, device_id=dev, device_id_type=MESH)

    def greet_mp(n, _):
        greet((dp, lax.rem(mp + n, N_MP)))
        return 0

    def greet_dp(n, _):
        greet((lax.rem(dp + n, N_DP), mp))
        return 0

    lax.fori_loop(1, N_MP, greet_mp, 0)
    lax.fori_loop(1, N_DP, greet_dp, 0)
    greet(((1 - h) * Z + z, rank_at(1 - yl, x, c)))

    rows_i = lax.broadcasted_iota(jnp.int32, (BLOCK, BLOCK), 0)
    cols_i = lax.broadcasted_iota(jnp.int32, (BLOCK, BLOCK), 1)
    diag = rows_i == cols_i

    def quantize(r):
        j = jnp.int32(0)
        for q in range(N_MP):
            j = j + jnp.where(rank_ref[q] == r, jnp.int32(q), jnp.int32(0))
        j = jnp.minimum(j, N_MP - 1)
        acc = jnp.zeros((8, BLOCK), jnp.float32)
        scales = []
        for k in range(ROWS // BLOCK):
            blk = w[j, pl.ds(k * BLOCK, BLOCK), :].astype(jnp.float32)
            peak = jnp.max(jnp.abs(blk), axis=1, keepdims=True)
            scale = (jnp.maximum(peak, floor_ratio / math.sqrt(D)) / 127.0).astype(jnp.bfloat16).astype(jnp.float32)
            scale = jnp.broadcast_to(scale, (BLOCK, BLOCK))
            quant = (blk / scale).astype(jnp.bfloat16)
            staged[r, pl.ds(k * BLOCK, BLOCK), :] = quant
            acc = acc + jnp.sum(quant.astype(jnp.float32).reshape(BLOCK // 8, 8, BLOCK), axis=0)
            scales.append(jnp.sum(jnp.where(diag, scale, 0.0), axis=0, keepdims=True))
        scales.append(jnp.zeros((PIECE - ROWS - len(scales), BLOCK), jnp.float32))
        staged[r, pl.ds(ROWS, PIECE - ROWS), :] = jnp.concatenate(scales, axis=0).astype(jnp.bfloat16)
        part[pl.ds(r, 1), :] = jnp.sum(acc, axis=0, keepdims=True)

    def quantize_step(m):
        def one(n, _):
            quantize(target(m, n // 2, lax.rem(n, 2)))
            return 0

        lax.fori_loop(0, 4, one, 0)

    def piece_copy(src, dst, sem_s, sem_r, dev):
        return pltpu.make_async_remote_copy(src, dst, sem_s, sem_r, device_id=dev, device_id_type=MESH)

    def await_recv(sem):
        piece_copy(staged.at[0], staged.at[0], send_x, sem, (dp, mp)).wait_recv()

    def along_x(m, cores):
        for cc in cores:
            to = lax.rem(c + cc, 2)
            s = 2 * m + cc
            dev = (dp, target(m, yl, to))
            piece_copy(staged.at[target(m, yl, to)], land.at[dp, mp], send_x, recv1.at[s, home], dev).start()
            piece_copy(staged.at[target(m, 1 - yl, to)], relay.at[s], send_x, recvr.at[s], dev).start()

    def spread(s, k):
        ref = land.at[lax.rem(k, 2) * Z + z, origin(s, k // 2)]
        piece_copy(ref, ref, send.at[s], recvz.at[0, s, k], (h * Z + z_at(1), mp)).start()
        piece_copy(ref, ref, send.at[s], recvz.at[1, s, k], (h * Z + z_at(3), mp)).start()

    def along_y(s, own=False):
        i = origin(s, yl)
        if not own:
            await_recv(recv1.at[s, home])
        ref = land.at[dp, i]
        piece_copy(ref, ref, send.at[s], recv1.at[s, home], ((1 - h) * Z + z, mp)).start()
        if not own:
            await_recv(recvr.at[s])
        ref = staged.at[rank_at(1 - yl, x, c)] if own else relay.at[s]
        for hh in (0, 1):
            dev = (lax.rem(h + hh, 2) * Z + z, rank_at(1 - yl, x, c))
            piece_copy(ref, land.at[dp, i], send.at[s], recv1.at[s, home], dev).start()
        spread(s, home)

    def spread_rest(s):
        for k in (yl * 2 + 1 - h, (1 - yl) * 2 + h, (1 - yl) * 2 + 1 - h):
            await_recv(recv1.at[s, k])
            spread(s, k)

    def onward(s):
        k = h * 2
        await_recv(recvz.at[0, s, k])
        ref = land.at[z_at(3), origin(s, h)]
        piece_copy(ref, ref, send.at[s], recvz.at[2, s, k], (h * Z + z_at(1), mp)).start()
        k = h * 2 + 1
        await_recv(recvz.at[1, s, k])
        ref = land.at[Z + z_at(1), origin(s, h)]
        piece_copy(ref, ref, send.at[s], recvz.at[2, s, k], (h * Z + z_at(3), mp)).start()

    def cross(s):
        for hs in (0, 1):
            k = h * 2 + hs
            await_recv(recvz.at[2, s, k])
            ref = land.at[hs * Z + z_at(2), origin(s, h)]
            piece_copy(ref, ref, send.at[s], recvz.at[2, s, k], ((1 - h) * Z + z, mp)).start()

    pltpu.make_async_copy(w, w, w_sem).wait()
    quantize_step(0)
    land[dp, mp, :, :] = staged[mp, :, :]
    pl.semaphore_wait(barrier, N_MP + N_DP - 1)
    along_x(0, (1,))
    along_y(0, own=True)

    def rest(m, _):
        quantize_step(m)
        along_x(m, (0, 1))
        return 0

    lax.fori_loop(1, 2, rest, 0)
    along_y(1)
    spread_rest(0)
    lax.fori_loop(2, 4, rest, 0)

    parts[dp, :, :] = part[...]

    def give(n, _):
        dev = (lax.rem(dp + n, N_DP), mp)
        piece_copy(part, parts.at[dp], send_s, sem_a, dev).start()
        return 0

    lax.fori_loop(1, N_DP, give, 0)

    along_y(2)
    spread_rest(1)
    onward(0)

    def main(s, _):
        along_y(s + 1)
        spread_rest(s)
        onward(s - 1)
        cross(s - 2)
        return 0

    lax.fori_loop(2, STEPS - 1, main, 0)
    spread_rest(STEPS - 1)

    pltpu.make_async_copy(parts.at[pl.ds(0, 7)], parts.at[pl.ds(0, 7)], sem_a).wait()
    whole = jnp.sum(jnp.sum(parts[...], axis=0), axis=1, keepdims=True)
    sums[mp, :, :] = jnp.broadcast_to(whole, (N_MP, BLOCK))

    onward(STEPS - 2)
    cross(STEPS - 3)

    def share(n, _):
        dev = (dp, lax.rem(mp + n, N_MP))
        piece_copy(sums.at[mp], sums.at[mp], send_s, sem_b, dev).start()
        return 0

    lax.fori_loop(1, N_MP, share, 0)
    onward(STEPS - 1)
    cross(STEPS - 2)
    cross(STEPS - 1)

    def finish(s, _):
        for k in (1, 2, 3):
            await_recv(recvz.at[0, s, lax.rem(h * 2 + k, 4)])
        for k in (1, 2, 3):
            await_recv(recvz.at[1, s, lax.rem(h * 2 + 1 + k, 4)])
        for k in (0, 1):
            await_recv(recvz.at[2, s, (1 - h) * 2 + k])
        return 0

    lax.fori_loop(0, STEPS, finish, 0)
    pltpu.make_async_copy(sums.at[pl.ds(0, 15)], sums.at[pl.ds(0, 15)], sem_b).wait()

    def sent(s, _):
        def one(n, _):
            piece_copy(staged.at[0], staged.at[0], send.at[s], w_sem, (dp, mp)).wait_send()
            return 0

        lax.fori_loop(0, 15, one, 0)
        return 0

    lax.fori_loop(0, STEPS, sent, 0)

    def sent_x(n, _):
        piece_copy(staged.at[0], staged.at[0], send_x, w_sem, (dp, mp)).wait_send()
        return 0

    lax.fori_loop(0, 14, sent_x, 0)

    def sent_small(n, _):
        piece_copy(part, part, send_s, w_sem, (dp, mp)).wait_send()
        return 0

    lax.fori_loop(0, 7 + 15, sent_small, 0)


def settle(rank_ref, land, sums, quant_out, scale_out, check_out, sem):
    for d in range(N_DP):
        for i in range(N_MP):
            pltpu.make_async_copy(
                land.at[d, i, pl.ds(0, ROWS), :],
                quant_out.at[pl.ds(d * ROWS, ROWS), pl.ds(i * BLOCK, BLOCK)],
                sem,
            ).start()
    n = PIECE - ROWS
    k_rows = ROWS // BLOCK
    out_i = lax.broadcasted_iota(jnp.int32, (k_rows * N_MP, N_MP * n), 0)
    in_i = lax.broadcasted_iota(jnp.int32, (k_rows * N_MP, N_MP * n), 1)
    pick = (in_i == lax.rem(out_i, N_MP) * n + out_i // N_MP).astype(jnp.bfloat16)
    eye = (
        lax.broadcasted_iota(jnp.int32, (BLOCK, BLOCK), 0) == lax.broadcasted_iota(jnp.int32, (BLOCK, BLOCK), 1)
    ).astype(jnp.bfloat16)

    def scales(d, _):
        rows = land[d, :, pl.ds(ROWS, n), :].reshape(N_MP * n, BLOCK)
        sorted_rows = jnp.dot(pick, rows, preferred_element_type=jnp.float32).astype(jnp.bfloat16)
        for k in range(k_rows):
            flat = lax.dot_general(
                eye, sorted_rows[k * N_MP : (k + 1) * N_MP], (((1,), (1,)), ((), ())), preferred_element_type=jnp.float32
            )
            scale_out[pl.ds(pl.multiple_of(d * ROWS + k * BLOCK, BLOCK), BLOCK), :] = flat.astype(jnp.bfloat16)
        return 0

    lax.fori_loop(0, N_DP, scales, 0)
    lane = lax.broadcasted_iota(jnp.int32, (N_MP, BLOCK), 1)
    total = jnp.zeros((N_MP, BLOCK), jnp.float32)
    for j in range(N_MP):
        total = total + jnp.where(lane == j, sums[:, rank_ref[j], :], 0.0)
    check_out[...] = total / (127.0 * math.sqrt(D * BLOCK))

    def done(n, _):
        pltpu.make_async_copy(
            land.at[0, 0, pl.ds(0, ROWS), :], quant_out.at[pl.ds(0, ROWS), pl.ds(0, BLOCK)], sem
        ).wait()
        return 0

    lax.fori_loop(0, N_DP * N_MP, done, 0)


def local(weight, rank_map):
    vmem = pl.BlockSpec(memory_space=pltpu.VMEM)
    smem = pl.BlockSpec(memory_space=pltpu.SMEM)
    hbm = pl.BlockSpec(memory_space=pl.ANY)
    dma = pltpu.SemaphoreType.DMA
    land, sums = pl.pallas_call(
        exchange,
        out_shape=(
            pltpu.VMEM((N_DP, N_MP, PIECE, BLOCK), jnp.bfloat16),
            pltpu.VMEM((N_MP, N_MP, BLOCK), jnp.float32),
        ),
        in_specs=[smem, pl.BlockSpec(memory_space=pltpu.HBM)],
        out_specs=(vmem, vmem),
        scratch_shapes=[
            pltpu.VMEM((N_MP, ROWS, BLOCK), jnp.bfloat16),
            pltpu.VMEM((N_MP, PIECE, BLOCK), jnp.bfloat16),
            pltpu.VMEM((STEPS, PIECE, BLOCK), jnp.bfloat16),
            pltpu.VMEM((N_MP, BLOCK), jnp.float32),
            pltpu.VMEM((N_DP, N_MP, BLOCK), jnp.float32),
            dma(()),
            dma((STEPS, 4)),
            dma((STEPS,)),
            dma((3, STEPS, 4)),
            dma((STEPS,)),
            dma(()),
            dma(()),
            dma(()),
            dma(()),
        ],
        compiler_params=pltpu.CompilerParams(collective_id=0, has_side_effects=True, vmem_limit_bytes=12 * MIB),
        name="exchange",
    )(rank_map, pltpu.with_memory_space_constraint(weight, pltpu.HBM))
    quant_out, scale_out, check = pl.pallas_call(
        settle,
        out_shape=(
            jax.ShapeDtypeStruct((D, N_MP * BLOCK), jnp.bfloat16),
            jax.ShapeDtypeStruct((D, N_MP), jnp.bfloat16),
            jax.ShapeDtypeStruct((N_MP, BLOCK), jnp.float32),
        ),
        in_specs=[smem, vmem, vmem],
        out_specs=(hbm, vmem, vmem),
        scratch_shapes=[dma(())],
        compiler_params=pltpu.CompilerParams(vmem_limit_bytes=12 * MIB),
        name="settle",
    )(rank_map, land, sums)
    return quant_out, scale_out, check[:, :N_MP].reshape(N_MP * N_MP)


def solution(mesh):
    return jax.shard_map(
        local,
        mesh=mesh,
        in_specs=(P("dp", "mp"), P()),
        out_specs=(P(None, "mp"), P(None, "mp"), P()),
        check_vma=False,
    )
```

```python
import functools
import math

import jax
import jax.numpy as jnp
from jax import lax
from jax.experimental import pallas as pl
from jax.experimental.pallas import tpu as pltpu
from jax.sharding import PartitionSpec as P

MESH = pl.DeviceIdType.MESH
D = 5120
floor_ratio = 0.25
BLOCK = 128
ROWS = 640
PIECE = 648
N_MP = 16
N_DP = 8
STEPS = 8
Z = 4
MIB = 1024 * 1024


def exchange(
    rank_hbm, w_hbm, land, sums, rank_ref, w, staged, relay, part, parts, rank_sem, w_sem, recv1, recvr, recvz, send, send_x, sem_a, sem_b, send_s
):
    dp = lax.axis_index("dp")
    mp = lax.axis_index("mp")
    h, z = dp // Z, lax.rem(dp, Z)
    yl, x, c = mp // 8, lax.rem(mp // 2, 4), lax.rem(mp, 2)
    home = yl * 2 + h

    pltpu.make_async_copy(rank_hbm, rank_ref, rank_sem).start()
    for q in range(N_MP):
        pltpu.make_async_copy(w_hbm.at[:, pl.ds(q * BLOCK, BLOCK)], w.at[q], w_sem).start()

    def z_at(dz):
        return lax.rem(z + dz, Z)

    def rank_at(yy, xx, cc):
        return yy * 8 + xx * 2 + cc

    def shift(m):
        return m + m // 2 - 2 * (m // 3)

    def target(m, yy, cc):
        return rank_at(yy, lax.rem(x + shift(m), 4), cc)

    def origin(s, yy):
        return rank_at(yy, lax.rem(x + 4 - shift(s // 2), 4), lax.rem(c + s, 2))

    barrier = pltpu.get_barrier_semaphore()

    def greet(dev):
        pl.semaphore_signal(barrier, inc=1, device_id=dev, device_id_type=MESH)

    def greet_mp(n, _):
        greet((dp, lax.rem(mp + n, N_MP)))
        return 0

    def greet_dp(n, _):
        greet((lax.rem(dp + n, N_DP), mp))
        return 0

    lax.fori_loop(1, N_MP, greet_mp, 0)
    lax.fori_loop(1, N_DP, greet_dp, 0)
    greet(((1 - h) * Z + z, rank_at(1 - yl, x, c)))

    rows_i = lax.broadcasted_iota(jnp.int32, (BLOCK, BLOCK), 0)
    cols_i = lax.broadcasted_iota(jnp.int32, (BLOCK, BLOCK), 1)
    diag = rows_i == cols_i

    def quantize(r):
        j = jnp.int32(0)
        for q in range(N_MP):
            j = j + jnp.where(rank_ref[q] == r, jnp.int32(q), jnp.int32(0))
        j = jnp.minimum(j, N_MP - 1)
        acc = jnp.zeros((8, BLOCK), jnp.float32)
        scales = []
        for k in range(ROWS // BLOCK):
            blk = w[j, pl.ds(k * BLOCK, BLOCK), :].astype(jnp.float32)
            peak = jnp.max(jnp.abs(blk), axis=1, keepdims=True)
            scale = (jnp.maximum(peak, floor_ratio / math.sqrt(D)) / 127.0).astype(jnp.bfloat16).astype(jnp.float32)
            scale = jnp.broadcast_to(scale, (BLOCK, BLOCK))
            quant = (blk / scale).astype(jnp.bfloat16)
            staged[r, pl.ds(k * BLOCK, BLOCK), :] = quant
            acc = acc + jnp.sum(quant.astype(jnp.float32).reshape(BLOCK // 8, 8, BLOCK), axis=0)
            scales.append(jnp.sum(jnp.where(diag, scale, 0.0), axis=0, keepdims=True))
        scales.append(jnp.zeros((PIECE - ROWS - len(scales), BLOCK), jnp.float32))
        staged[r, pl.ds(ROWS, PIECE - ROWS), :] = jnp.concatenate(scales, axis=0).astype(jnp.bfloat16)
        part[pl.ds(r, 1), :] = jnp.sum(acc, axis=0, keepdims=True)

    def quantize_step(m):
        def one(n, _):
            quantize(target(m, n // 2, lax.rem(n, 2)))
            return 0

        lax.fori_loop(0, 4, one, 0)

    def thin(s, way):
        return jnp.logical_or(s == 1 + way, s == 3 + way)

    def piece_copy(src, dst, sem_s, sem_r, dev):
        return pltpu.make_async_remote_copy(src, dst, sem_s, sem_r, device_id=dev, device_id_type=MESH)

    def await_recv(sem):
        piece_copy(staged.at[0], staged.at[0], send_x, sem, (dp, mp)).wait_recv()

    def along_x(m, cores):
        for cc in cores:
            to = lax.rem(c + cc, 2)
            s = 2 * m + cc
            dev = (dp, target(m, yl, to))
            piece_copy(staged.at[target(m, yl, to)], land.at[dp, mp], send_x, recv1.at[s, home], dev).start()
            piece_copy(staged.at[target(m, 1 - yl, to)], relay.at[s], send_x, recvr.at[s], dev).start()

    def spread(s, k):
        ref = land.at[lax.rem(k, 2) * Z + z, origin(s, k // 2)]
        for way, dz in ((0, 1), (1, 3)):

            @pl.when(jnp.logical_or(k // 2 == h, jnp.logical_not(thin(s, way))))
            def _():
                piece_copy(ref, ref, send.at[s], recvz.at[way, s, k], (h * Z + z_at(dz), mp)).start()

    def over_y(s, own=False):
        if not own:
            await_recv(recv1.at[s, home])
        ref = land.at[dp, origin(s, yl)]
        piece_copy(ref, ref, send.at[s], recv1.at[s, home], ((1 - h) * Z + z, mp)).start()
        spread(s, home)

    def beside_y(s, own=False):
        if not own:
            await_recv(recvr.at[s])
        ref = staged.at[rank_at(1 - yl, x, c)] if own else relay.at[s]
        for hh in (0, 1):
            dev = (lax.rem(h + hh, 2) * Z + z, rank_at(1 - yl, x, c))
            piece_copy(ref, land.at[dp, origin(s, yl)], send.at[s], recv1.at[s, home], dev).start()

    def along_y(s):
        over_y(s)
        beside_y(s)

    def spread_rest(s):
        for k in (yl * 2 + 1 - h, (1 - yl) * 2 + h, (1 - yl) * 2 + 1 - h):
            await_recv(recv1.at[s, k])
            spread(s, k)

    def arrived(way, s, k):
        block = z_at(2) if way == 2 else (z_at(3) if way == 0 else z_at(1))
        return land.at[lax.rem(k, 2) * Z + block, origin(s, k // 2)]

    def onward(s, rows=(0,)):
        for row in rows:
            for way, dz in ((0, 1), (1, 3)):
                k = lax.rem(h + row, 2) * 2 + way
                await_recv(recvz.at[way, s, k])
                ref = arrived(way, s, k)
                piece_copy(ref, ref, send.at[s], recvz.at[2, s, k], (h * Z + z_at(dz), mp)).start()

    def over(way, s, k):
        ref = arrived(way, s, k)
        piece_copy(ref, ref, send.at[s], recvz.at[way, s, k], ((1 - h) * Z + z, mp)).start()

    def cross_near(s):
        for way in (0, 1):

            @pl.when(thin(s, way))
            def _():
                over(way, s, h * 2 + way)
                await_recv(recvz.at[way, s, h * 2 + 1 - way])
                over(way, s, h * 2 + 1 - way)

    def cross(s):
        for hs in (0, 1):
            await_recv(recvz.at[2, s, h * 2 + hs])
            over(2, s, h * 2 + hs)

    pltpu.make_async_copy(rank_hbm, rank_ref, rank_sem).wait()
    pltpu.make_async_copy(w, w, w_sem).wait()
    quantize(mp)
    land[dp, mp, :, :] = staged[mp, :, :]
    pl.semaphore_wait(barrier, N_MP + N_DP - 1)
    over_y(0, own=True)
    quantize(target(0, 1 - yl, c))
    beside_y(0, own=True)
    quantize(target(0, yl, 1 - c))
    quantize(target(0, 1 - yl, 1 - c))
    along_x(0, (1,))

    def rest(m, _):
        quantize_step(m)
        along_x(m, (0, 1))
        return 0

    lax.fori_loop(1, 2, rest, 0)
    along_y(1)
    spread_rest(0)
    lax.fori_loop(2, 4, rest, 0)

    parts[dp, :, :] = part[...]

    def give(n, _):
        dev = (lax.rem(dp + n, N_DP), mp)
        piece_copy(part, parts.at[dp], send_s, sem_a, dev).start()
        return 0

    lax.fori_loop(1, N_DP, give, 0)

    along_y(2)
    spread_rest(1)
    onward(0)

    def main(s, _):
        along_y(s + 1)
        spread_rest(s)
        onward(s - 1)
        cross_near(s - 1)
        cross(s - 2)
        return 0

    lax.fori_loop(2, STEPS - 1, main, 0)
    spread_rest(STEPS - 1)

    pltpu.make_async_copy(parts.at[pl.ds(0, 7)], parts.at[pl.ds(0, 7)], sem_a).wait()
    whole = jnp.sum(jnp.sum(parts[...], axis=0), axis=1, keepdims=True)
    sums[mp, :, :] = jnp.broadcast_to(whole, (N_MP, BLOCK))

    onward(STEPS - 2)
    cross(STEPS - 3)

    def share(n, _):
        dev = (dp, lax.rem(mp + n, N_MP))
        piece_copy(sums.at[mp], sums.at[mp], send_s, sem_b, dev).start()
        return 0

    lax.fori_loop(1, N_MP, share, 0)
    onward(STEPS - 1, rows=(0, 1))
    cross(STEPS - 2)

    def finish(s, _):
        for way in (0, 1):

            @pl.when(jnp.logical_not(thin(s, way)))
            def _():
                await_recv(recvz.at[way, s, h * 2 + 1 - way])

            @pl.when(s < STEPS - 1)
            def _():
                await_recv(recvz.at[way, s, (1 - h) * 2 + way])

            await_recv(recvz.at[way, s, (1 - h) * 2 + 1 - way])
            await_recv(recvz.at[2, s, (1 - h) * 2 + way])
        return 0

    lax.fori_loop(0, STEPS, finish, 0)
    await_recv(recvz.at[2, STEPS - 1, h * 2])
    await_recv(recvz.at[2, STEPS - 1, h * 2 + 1])
    pltpu.make_async_copy(sums.at[pl.ds(0, 15)], sums.at[pl.ds(0, 15)], sem_b).wait()

    def sent(s, _):
        def one(n, _):
            piece_copy(staged.at[0], staged.at[0], send.at[s], w_sem, (dp, mp)).wait_send()
            return 0

        lax.fori_loop(0, 15, one, 0)
        return 0

    lax.fori_loop(0, STEPS, sent, 0)

    def sent_x(n, _):
        piece_copy(staged.at[0], staged.at[0], send_x, w_sem, (dp, mp)).wait_send()
        return 0

    lax.fori_loop(0, 14, sent_x, 0)

    def sent_small(n, _):
        piece_copy(part, part, send_s, w_sem, (dp, mp)).wait_send()
        return 0

    lax.fori_loop(0, 7 + 15, sent_small, 0)


def settle(rank_hbm, land, sums, quant_out, scale_out, check_out, rank_ref, rank_sem, sem):
    pltpu.make_async_copy(rank_hbm, rank_ref, rank_sem).start()
    for d in range(N_DP):
        for i in range(N_MP):
            pltpu.make_async_copy(
                land.at[d, i, pl.ds(0, ROWS), :],
                quant_out.at[pl.ds(d * ROWS, ROWS), pl.ds(i * BLOCK, BLOCK)],
                sem,
            ).start()
    n = PIECE - ROWS
    k_rows = ROWS // BLOCK
    out_i = lax.broadcasted_iota(jnp.int32, (k_rows * N_MP, N_MP * n), 0)
    in_i = lax.broadcasted_iota(jnp.int32, (k_rows * N_MP, N_MP * n), 1)
    pick = (in_i == lax.rem(out_i, N_MP) * n + out_i // N_MP).astype(jnp.bfloat16)

    for d in range(N_DP):
        rows = land[d, :, pl.ds(ROWS, n), :].reshape(N_MP * n, BLOCK)
        ordered = jnp.dot(pick, rows, preferred_element_type=jnp.float32).astype(jnp.bfloat16)
        for k in range(k_rows):
            scale_out[:, pl.ds(d * ROWS + k * BLOCK, BLOCK)] = ordered[k * N_MP : (k + 1) * N_MP]

    pltpu.make_async_copy(rank_hbm, rank_ref, rank_sem).wait()
    row = lax.broadcasted_iota(jnp.int32, (N_MP, BLOCK), 0)
    lane = lax.broadcasted_iota(jnp.int32, (N_MP, BLOCK), 1)
    total = jnp.zeros((N_MP, BLOCK), jnp.float32)
    for j in range(N_MP):
        total = total + jnp.where(lane == lax.rem(row, 8) * N_MP + j, sums[:, rank_ref[j], :], 0.0)
    total = total / (127.0 * math.sqrt(D * BLOCK))
    for p in (0, 1):
        check_out[pl.ds(p, 1), :] = jnp.sum(total[p * 8 : (p + 1) * 8], axis=0, keepdims=True)

    def done(n, _):
        pltpu.make_async_copy(
            land.at[0, 0, pl.ds(0, ROWS), :], quant_out.at[pl.ds(0, ROWS), pl.ds(0, BLOCK)], sem
        ).wait()
        return 0

    lax.fori_loop(0, N_DP * N_MP, done, 0)


def local(weight, rank_map):
    vmem = pl.BlockSpec(memory_space=pltpu.VMEM)
    hbm = pl.BlockSpec(memory_space=pltpu.HBM)
    rank_map = pltpu.with_memory_space_constraint(rank_map, pltpu.HBM)
    weight = pltpu.with_memory_space_constraint(weight, pltpu.HBM)
    dma = pltpu.SemaphoreType.DMA
    land, sums = pl.pallas_call(
        exchange,
        out_shape=(
            pltpu.VMEM((N_DP, N_MP, PIECE, BLOCK), jnp.bfloat16),
            pltpu.VMEM((N_MP, N_MP, BLOCK), jnp.float32),
        ),
        in_specs=[hbm, hbm],
        out_specs=(vmem, vmem),
        scratch_shapes=[
            pltpu.SMEM((N_MP,), jnp.int32),
            pltpu.VMEM((N_MP, ROWS, BLOCK), jnp.bfloat16),
            pltpu.VMEM((N_MP, PIECE, BLOCK), jnp.bfloat16),
            pltpu.VMEM((STEPS, PIECE, BLOCK), jnp.bfloat16),
            pltpu.VMEM((N_MP, BLOCK), jnp.float32),
            pltpu.VMEM((N_DP, N_MP, BLOCK), jnp.float32),
            dma(()),
            dma(()),
            dma((STEPS, 4)),
            dma((STEPS,)),
            dma((3, STEPS, 4)),
            dma((STEPS,)),
            dma(()),
            dma(()),
            dma(()),
            dma(()),
        ],
        compiler_params=pltpu.CompilerParams(collective_id=0, has_side_effects=True, vmem_limit_bytes=12 * MIB),
        name="exchange",
    )(rank_map, weight)
    quant_out, scale_out, check = pl.pallas_call(
        settle,
        out_shape=(
            jax.ShapeDtypeStruct((D, N_MP * BLOCK), jnp.bfloat16),
            jax.ShapeDtypeStruct((N_MP, D), jnp.bfloat16),
            jax.ShapeDtypeStruct((2, BLOCK), jnp.float32),
        ),
        in_specs=[hbm, vmem, vmem],
        out_specs=(hbm, vmem, vmem),
        scratch_shapes=[pltpu.SMEM((N_MP,), jnp.int32), dma(()), dma(())],
        compiler_params=pltpu.CompilerParams(vmem_limit_bytes=12 * MIB),
        name="settle",
    )(rank_map, land, sums)
    return quant_out, scale_out.T, check.reshape(2 * BLOCK)


def solution(mesh):
    return jax.shard_map(
        local,
        mesh=mesh,
        in_specs=(P("dp", "mp"), P()),
        out_specs=(P(None, "mp"), P(None, "mp"), P()),
        check_vma=False,
    )
```

```python
import functools
import math

import jax
import jax.numpy as jnp
from jax import lax
from jax.experimental import pallas as pl
from jax.experimental.pallas import tpu as pltpu
from jax.sharding import PartitionSpec as P

MESH = pl.DeviceIdType.MESH
D = 5120
floor_ratio = 0.25
BLOCK = 128
ROWS = 640
PIECE = 648
N_MP = 16
N_DP = 8
STEPS = 8
Z = 4
MIB = 1024 * 1024
THIN = (
    (1, 0, 0),
    (1, 0, 1),
    (2, 1, 0),
    (2, 1, 1),
    (3, 0, 0),
    (3, 0, 1),
    (4, 1, 0),
    (4, 1, 1),
)
PLAIN = (7,)
EARLY = (
    ("Y", 2),
    ("Y", 3),
    ("R", 1),
    ("O", 0),
    ("Y", 4),
    ("R", 2),
    ("O", 1),
    ("C", 0),
    ("Y", 5),
    ("R", 3),
    ("O", 2),
    ("C", 1),
    ("Y", 6),
    ("R", 4),
    ("O", 3),
    ("C", 2),
    ("Y", 7),
    ("R", 5),
    ("O", 4),
    ("C", 3),
    ("R", 6),
    ("O", 5),
    ("C", 4),
    ("R", 7),
)
LATE = (
    ("O", 6),
    ("C", 5),
    ("O", 7),
    ("C", 6),
)


def exchange(
    rank_hbm, w_hbm, land, sums, rank_ref, w, staged, relay, part, parts, rank_sem, w_sem, recv1, recvr, recvz, send, send_x, sem_a, sem_b, send_s
):
    dp = lax.axis_index("dp")
    mp = lax.axis_index("mp")
    h, z = dp // Z, lax.rem(dp, Z)
    yl, x, c = mp // 8, lax.rem(mp // 2, 4), lax.rem(mp, 2)
    home = yl * 2 + h

    pltpu.make_async_copy(rank_hbm, rank_ref, rank_sem).start()
    for q in range(N_MP):
        pltpu.make_async_copy(w_hbm.at[:, pl.ds(q * BLOCK, BLOCK)], w.at[q], w_sem).start()

    def z_at(dz):
        return lax.rem(z + dz, Z)

    def rank_at(yy, xx, cc):
        return yy * 8 + xx * 2 + cc

    def shift(m):
        return m + m // 2 - 2 * (m // 3)

    def target(m, yy, cc):
        return rank_at(yy, lax.rem(x + shift(m), 4), cc)

    def origin(s, yy):
        return rank_at(yy, lax.rem(x + 4 - shift(s // 2), 4), lax.rem(c + s, 2))

    barrier = pltpu.get_barrier_semaphore()

    def greet(dev):
        pl.semaphore_signal(barrier, inc=1, device_id=dev, device_id_type=MESH)

    def greet_mp(n, _):
        greet((dp, lax.rem(mp + n, N_MP)))
        return 0

    def greet_dp(n, _):
        greet((lax.rem(dp + n, N_DP), mp))
        return 0

    lax.fori_loop(1, N_MP, greet_mp, 0)
    lax.fori_loop(1, N_DP, greet_dp, 0)
    greet(((1 - h) * Z + z, rank_at(1 - yl, x, c)))

    rows_i = lax.broadcasted_iota(jnp.int32, (BLOCK, BLOCK), 0)
    cols_i = lax.broadcasted_iota(jnp.int32, (BLOCK, BLOCK), 1)
    diag = rows_i == cols_i

    def quantize(r):
        j = jnp.int32(0)
        for q in range(N_MP):
            j = j + jnp.where(rank_ref[q] == r, jnp.int32(q), jnp.int32(0))
        j = jnp.minimum(j, N_MP - 1)
        acc = jnp.zeros((8, BLOCK), jnp.float32)
        scales = []
        for k in range(ROWS // BLOCK):
            blk = w[j, pl.ds(k * BLOCK, BLOCK), :].astype(jnp.float32)
            peak = jnp.max(jnp.abs(blk), axis=1, keepdims=True)
            scale = (jnp.maximum(peak, floor_ratio / math.sqrt(D)) / 127.0).astype(jnp.bfloat16).astype(jnp.float32)
            scale = jnp.broadcast_to(scale, (BLOCK, BLOCK))
            quant = (blk / scale).astype(jnp.bfloat16)
            staged[r, pl.ds(k * BLOCK, BLOCK), :] = quant
            acc = acc + jnp.sum(quant.astype(jnp.float32).reshape(BLOCK // 8, 8, BLOCK), axis=0)
            scales.append(jnp.sum(jnp.where(diag, scale, 0.0), axis=0, keepdims=True))
        scales.append(jnp.zeros((PIECE - ROWS - len(scales), BLOCK), jnp.float32))
        staged[r, pl.ds(ROWS, PIECE - ROWS), :] = jnp.concatenate(scales, axis=0).astype(jnp.bfloat16)
        part[pl.ds(r, 1), :] = jnp.sum(acc, axis=0, keepdims=True)

    def quantize_step(m):
        def one(n, _):
            quantize(target(m, n // 2, lax.rem(n, 2)))
            return 0

        lax.fori_loop(0, 4, one, 0)

    def piece_copy(src, dst, sem_s, sem_r, dev):
        return pltpu.make_async_remote_copy(src, dst, sem_s, sem_r, device_id=dev, device_id_type=MESH)

    def await_recv(sem):
        piece_copy(staged.at[0], staged.at[0], send_x, sem, (dp, mp)).wait_recv()

    def along_x(m, cores):
        for cc in cores:
            to = lax.rem(c + cc, 2)
            s = 2 * m + cc
            dev = (dp, target(m, yl, to))
            piece_copy(staged.at[target(m, yl, to)], land.at[dp, mp], send_x, recv1.at[s, home], dev).start()
            piece_copy(staged.at[target(m, 1 - yl, to)], relay.at[s], send_x, recvr.at[s], dev).start()

    def spread(s, k):
        ref = land.at[lax.rem(k, 2) * Z + z, origin(s, k // 2)]
        for way, dz in ((0, 1), (1, 3)):
            send_z = functools.partial(
                piece_copy, ref, ref, send.at[s], recvz.at[way, s, k], (h * Z + z_at(dz), mp)
            )
            thin = [hs for hs in (0, 1) if (s, way, hs) in THIN]
            if not thin:
                send_z().start()
            else:
                keep = k // 2 == h
                if len(thin) == 1:
                    keep = jnp.logical_or(keep, lax.rem(k, 2) != thin[0])

                @pl.when(keep)
                def _():
                    send_z().start()

    def over_y(s, own=False):
        if not own:
            await_recv(recv1.at[s, home])
        ref = land.at[dp, origin(s, yl)]
        piece_copy(ref, ref, send.at[s], recv1.at[s, home], ((1 - h) * Z + z, mp)).start()
        spread(s, home)

    def beside_y(s, own=False):
        if not own:
            await_recv(recvr.at[s])
        ref = staged.at[rank_at(1 - yl, x, c)] if own else relay.at[s]
        for hh in (0, 1):
            dev = (lax.rem(h + hh, 2) * Z + z, rank_at(1 - yl, x, c))
            piece_copy(ref, land.at[dp, origin(s, yl)], send.at[s], recv1.at[s, home], dev).start()

    def along_y(s):
        over_y(s)
        beside_y(s)

    def spread_rest(s):
        for k in (yl * 2 + 1 - h, (1 - yl) * 2 + h, (1 - yl) * 2 + 1 - h):
            await_recv(recv1.at[s, k])
            spread(s, k)

    def arrived(way, s, k):
        block = z_at(2) if way == 2 else (z_at(3) if way == 0 else z_at(1))
        return land.at[lax.rem(k, 2) * Z + block, origin(s, k // 2)]

    def onward(s):
        for row in (0, 1) if s in PLAIN else (0,):
            for way, dz in ((0, 1), (1, 3)):
                k = lax.rem(h + row, 2) * 2 + way
                await_recv(recvz.at[way, s, k])
                ref = arrived(way, s, k)
                piece_copy(ref, ref, send.at[s], recvz.at[2, s, k], (h * Z + z_at(dz), mp)).start()
        for way in (0, 1):
            for hs in (way, 1 - way):
                if (s, way, hs) in THIN:
                    if hs != way:
                        await_recv(recvz.at[way, s, h * 2 + hs])
                    over(way, s, h * 2 + hs)

    def over(way, s, k):
        ref = arrived(way, s, k)
        piece_copy(ref, ref, send.at[s], recvz.at[way, s, k], ((1 - h) * Z + z, mp)).start()

    def cross(s):
        if s in PLAIN:
            return
        for hs in (0, 1):
            await_recv(recvz.at[2, s, h * 2 + hs])
            over(2, s, h * 2 + hs)

    pltpu.make_async_copy(rank_hbm, rank_ref, rank_sem).wait()
    pltpu.make_async_copy(w, w, w_sem).wait()
    quantize(mp)
    land[dp, mp, :, :] = staged[mp, :, :]
    pl.semaphore_wait(barrier, N_MP + N_DP - 1)
    over_y(0, own=True)
    quantize(target(0, 1 - yl, c))
    beside_y(0, own=True)
    quantize(target(0, yl, 1 - c))
    quantize(target(0, 1 - yl, 1 - c))
    along_x(0, (1,))

    def rest(m, _):
        quantize_step(m)
        along_x(m, (0, 1))
        return 0

    lax.fori_loop(1, 2, rest, 0)
    along_y(1)
    spread_rest(0)
    lax.fori_loop(2, 4, rest, 0)

    parts[dp, :, :] = part[...]

    def give(n, _):
        dev = (lax.rem(dp + n, N_DP), mp)
        piece_copy(part, parts.at[dp], send_s, sem_a, dev).start()
        return 0

    lax.fori_loop(1, N_DP, give, 0)

    steps = {"Y": along_y, "R": spread_rest, "O": onward, "C": cross}
    for name, step in EARLY:
        steps[name](step)

    pltpu.make_async_copy(parts.at[pl.ds(0, 7)], parts.at[pl.ds(0, 7)], sem_a).wait()
    whole = jnp.sum(jnp.sum(parts[...], axis=0), axis=1, keepdims=True)
    sums[mp, :, :] = jnp.broadcast_to(whole, (N_MP, BLOCK))

    def share(n, _):
        dev = (dp, lax.rem(mp + n, N_MP))
        piece_copy(sums.at[mp], sums.at[mp], send_s, sem_b, dev).start()
        return 0

    lax.fori_loop(1, N_MP, share, 0)
    for name, step in LATE:
        steps[name](step)
    def sent(sem, n, ref):
        def one(_, carry):
            piece_copy(ref, ref, sem, w_sem, (dp, mp)).wait_send()
            return carry

        lax.fori_loop(0, n, one, 0)

    sent(send_x, 14, staged.at[0])
    sent(send_s, 7 + 15, part)
    for step in range(STEPS):
        sent(send.at[step], 15, staged.at[0])
    for step in range(STEPS):
        for way in (0, 1):
            if (step, way, 1 - way) not in THIN:
                await_recv(recvz.at[way, step, h * 2 + 1 - way])
            if step not in PLAIN:
                await_recv(recvz.at[way, step, (1 - h) * 2 + way])
            else:
                await_recv(recvz.at[2, step, h * 2 + way])
            await_recv(recvz.at[way, step, (1 - h) * 2 + 1 - way])
            await_recv(recvz.at[2, step, (1 - h) * 2 + way])
    pltpu.make_async_copy(sums.at[pl.ds(0, 15)], sums.at[pl.ds(0, 15)], sem_b).wait()


def settle(rank_hbm, land, sums, quant_out, scale_hbm, check_hbm, rank_ref, scale_out, check_out, rank_sem, sem, sem_s):
    pltpu.make_async_copy(rank_hbm, rank_ref, rank_sem).start()
    for d in range(N_DP):
        for i in range(N_MP):
            pltpu.make_async_copy(
                land.at[d, i, pl.ds(0, ROWS), :],
                quant_out.at[pl.ds(d * ROWS, ROWS), pl.ds(i * BLOCK, BLOCK)],
                sem,
            ).start()
    n = PIECE - ROWS
    k_rows = ROWS // BLOCK
    out_i = lax.broadcasted_iota(jnp.int32, (k_rows * N_MP, N_MP * n), 0)
    in_i = lax.broadcasted_iota(jnp.int32, (k_rows * N_MP, N_MP * n), 1)
    pick = (in_i == lax.rem(out_i, N_MP) * n + out_i // N_MP).astype(jnp.bfloat16)

    for d in range(N_DP):
        rows = land[d, :, pl.ds(ROWS, n), :].reshape(N_MP * n, BLOCK)
        ordered = jnp.dot(pick, rows, preferred_element_type=jnp.float32).astype(jnp.bfloat16)
        for k in range(k_rows):
            scale_out[:, pl.ds(d * ROWS + k * BLOCK, BLOCK)] = ordered[k * N_MP : (k + 1) * N_MP]

    pltpu.make_async_copy(rank_hbm, rank_ref, rank_sem).wait()
    row = lax.broadcasted_iota(jnp.int32, (N_MP, BLOCK), 0)
    lane = lax.broadcasted_iota(jnp.int32, (N_MP, BLOCK), 1)
    total = jnp.zeros((N_MP, BLOCK), jnp.float32)
    for j in range(N_MP):
        total = total + jnp.where(lane == lax.rem(row, 8) * N_MP + j, sums[:, rank_ref[j], :], 0.0)
    total = total / (127.0 * math.sqrt(D * BLOCK))
    for p in (0, 1):
        check_out[pl.ds(p, 1), :] = jnp.sum(total[p * 8 : (p + 1) * 8], axis=0, keepdims=True)

    small = (pltpu.make_async_copy(scale_out, scale_hbm, sem_s), pltpu.make_async_copy(check_out, check_hbm, rank_sem))
    for copy in small:
        copy.start()

    def done(n, _):
        pltpu.make_async_copy(
            land.at[0, 0, pl.ds(0, ROWS), :], quant_out.at[pl.ds(0, ROWS), pl.ds(0, BLOCK)], sem
        ).wait()
        return 0

    lax.fori_loop(0, N_DP * N_MP, done, 0)
    for copy in small:
        copy.wait()


def local(weight, rank_map):
    vmem = pl.BlockSpec(memory_space=pltpu.VMEM)
    hbm = pl.BlockSpec(memory_space=pltpu.HBM)
    rank_map = pltpu.with_memory_space_constraint(rank_map, pltpu.HBM)
    weight = pltpu.with_memory_space_constraint(weight, pltpu.HBM)
    dma = pltpu.SemaphoreType.DMA
    land, sums = pl.pallas_call(
        exchange,
        out_shape=(
            pltpu.VMEM((N_DP, N_MP, PIECE, BLOCK), jnp.bfloat16),
            pltpu.VMEM((N_MP, N_MP, BLOCK), jnp.float32),
        ),
        in_specs=[hbm, hbm],
        out_specs=(vmem, vmem),
        scratch_shapes=[
            pltpu.SMEM((N_MP,), jnp.int32),
            pltpu.VMEM((N_MP, ROWS, BLOCK), jnp.bfloat16),
            pltpu.VMEM((N_MP, PIECE, BLOCK), jnp.bfloat16),
            pltpu.VMEM((STEPS, PIECE, BLOCK), jnp.bfloat16),
            pltpu.VMEM((N_MP, BLOCK), jnp.float32),
            pltpu.VMEM((N_DP, N_MP, BLOCK), jnp.float32),
            dma(()),
            dma(()),
            dma((STEPS, 4)),
            dma((STEPS,)),
            dma((3, STEPS, 4)),
            dma((STEPS,)),
            dma(()),
            dma(()),
            dma(()),
            dma(()),
        ],
        compiler_params=pltpu.CompilerParams(collective_id=0, has_side_effects=True, vmem_limit_bytes=12 * MIB),
        name="exchange",
    )(rank_map, weight)
    quant_out, scale_out, check = pl.pallas_call(
        settle,
        out_shape=(
            pltpu.HBM((D, N_MP * BLOCK), jnp.bfloat16),
            pltpu.HBM((N_MP, D), jnp.bfloat16),
            pltpu.HBM((2, BLOCK), jnp.float32),
        ),
        in_specs=[hbm, vmem, vmem],
        out_specs=(hbm, hbm, hbm),
        scratch_shapes=[
            pltpu.SMEM((N_MP,), jnp.int32),
            pltpu.VMEM((N_MP, D), jnp.bfloat16),
            pltpu.VMEM((2, BLOCK), jnp.float32),
            dma(()),
            dma(()),
            dma(()),
        ],
        compiler_params=pltpu.CompilerParams(vmem_limit_bytes=12 * MIB),
        name="settle",
    )(rank_map, land, sums)
    return quant_out, scale_out.T, check.reshape(2 * BLOCK)


def solution(mesh):
    return jax.shard_map(
        local,
        mesh=mesh,
        in_specs=(P("dp", "mp"), P()),
        out_specs=(P(None, "mp"), P(None, "mp"), P()),
        check_vma=False,
    )
```

```python
import functools
import math

import jax
import jax.numpy as jnp
from jax import lax
from jax.experimental import pallas as pl
from jax.experimental.pallas import tpu as pltpu
from jax.sharding import PartitionSpec as P

MESH = pl.DeviceIdType.MESH
D = 5120
floor_ratio = 0.25
BLOCK = 128
ROWS = 640
PIECE = 648
N_MP = 16
N_DP = 8
STEPS = 8
Z = 4
MIB = 1024 * 1024
THIN = (
    (1, 0, 0),
    (1, 0, 1),
    (2, 1, 0),
    (2, 1, 1),
    (3, 0, 0),
    (3, 0, 1),
    (4, 1, 0),
)
PLAIN = (7,)
EARLY = (
    ("Y", 2),
    ("R", 1),
    ("Y", 3),
    ("O", 0),
    ("Y", 4),
    ("R", 2),
    ("O", 1),
    ("C", 0),
    ("Y", 5),
    ("R", 3),
    ("O", 2),
    ("C", 1),
    ("Y", 6),
    ("R", 4),
    ("O", 3),
    ("C", 2),
    ("Y", 7),
    ("R", 5),
    ("O", 4),
    ("C", 3),
    ("R", 6),
    ("O", 5),
    ("C", 4),
    ("O", 6),
    ("C", 5),
    ("R", 7),
)
LATE = (
    ("C", 6),
    ("O", 7),
)


def exchange(
    rank_hbm, w_hbm, land, sums, rank_ref, w, staged, relay, part, parts, rank_sem, w_sem, recv1, recvr, recvz, send, send_x, sem_a, sem_b, send_s
):
    dp = lax.axis_index("dp")
    mp = lax.axis_index("mp")
    h, z = dp // Z, lax.rem(dp, Z)
    yl, x, c = mp // 8, lax.rem(mp // 2, 4), lax.rem(mp, 2)
    home = yl * 2 + h

    pltpu.make_async_copy(rank_hbm, rank_ref, rank_sem).start()
    for q in range(N_MP):
        pltpu.make_async_copy(w_hbm.at[:, pl.ds(q * BLOCK, BLOCK)], w.at[q], w_sem).start()

    def z_at(dz):
        return lax.rem(z + dz, Z)

    def rank_at(yy, xx, cc):
        return yy * 8 + xx * 2 + cc

    def shift(m):
        return m + m // 2 - 2 * (m // 3)

    def target(m, yy, cc):
        return rank_at(yy, lax.rem(x + shift(m), 4), cc)

    def origin(s, yy):
        return rank_at(yy, lax.rem(x + 4 - shift(s // 2), 4), lax.rem(c + s, 2))

    barrier = pltpu.get_barrier_semaphore()

    def greet(dev):
        pl.semaphore_signal(barrier, inc=1, device_id=dev, device_id_type=MESH)

    def greet_mp(n, _):
        greet((dp, lax.rem(mp + n, N_MP)))
        return 0

    def greet_dp(n, _):
        greet((lax.rem(dp + n, N_DP), mp))
        return 0

    lax.fori_loop(1, N_MP, greet_mp, 0)
    lax.fori_loop(1, N_DP, greet_dp, 0)
    greet(((1 - h) * Z + z, rank_at(1 - yl, x, c)))

    rows_i = lax.broadcasted_iota(jnp.int32, (BLOCK, BLOCK), 0)
    cols_i = lax.broadcasted_iota(jnp.int32, (BLOCK, BLOCK), 1)
    diag = rows_i == cols_i

    def quantize(r):
        j = jnp.int32(0)
        for q in range(N_MP):
            j = j + jnp.where(rank_ref[q] == r, jnp.int32(q), jnp.int32(0))
        j = jnp.minimum(j, N_MP - 1)
        acc = jnp.zeros((8, BLOCK), jnp.float32)
        scales = []
        for k in range(ROWS // BLOCK):
            blk = w[j, pl.ds(k * BLOCK, BLOCK), :].astype(jnp.float32)
            peak = jnp.max(jnp.abs(blk), axis=1, keepdims=True)
            scale = (jnp.maximum(peak, floor_ratio / math.sqrt(D)) / 127.0).astype(jnp.bfloat16).astype(jnp.float32)
            scale = jnp.broadcast_to(scale, (BLOCK, BLOCK))
            quant = (blk / scale).astype(jnp.bfloat16)
            staged[r, pl.ds(k * BLOCK, BLOCK), :] = quant
            acc = acc + jnp.sum(quant.astype(jnp.float32).reshape(BLOCK // 8, 8, BLOCK), axis=0)
            scales.append(jnp.sum(jnp.where(diag, scale, 0.0), axis=0, keepdims=True))
        scales.append(jnp.zeros((PIECE - ROWS - len(scales), BLOCK), jnp.float32))
        staged[r, pl.ds(ROWS, PIECE - ROWS), :] = jnp.concatenate(scales, axis=0).astype(jnp.bfloat16)
        part[pl.ds(r, 1), :] = jnp.sum(acc, axis=0, keepdims=True)

    def quantize_step(m):
        def one(n, _):
            quantize(target(m, n // 2, lax.rem(n, 2)))
            return 0

        lax.fori_loop(0, 4, one, 0)

    def piece_copy(src, dst, sem_s, sem_r, dev):
        return pltpu.make_async_remote_copy(src, dst, sem_s, sem_r, device_id=dev, device_id_type=MESH)

    def await_recv(sem):
        piece_copy(staged.at[0], staged.at[0], send_x, sem, (dp, mp)).wait_recv()

    def along_x(m, cores):
        for cc in cores:
            to = lax.rem(c + cc, 2)
            s = 2 * m + cc
            dev = (dp, target(m, yl, to))
            piece_copy(staged.at[target(m, yl, to)], land.at[dp, mp], send_x, recv1.at[s, home], dev).start()
            piece_copy(staged.at[target(m, 1 - yl, to)], relay.at[s], send_x, recvr.at[s], dev).start()

    def spread(s, k):
        ref = land.at[lax.rem(k, 2) * Z + z, origin(s, k // 2)]
        for way, dz in ((0, 1), (1, 3)):
            send_z = functools.partial(
                piece_copy, ref, ref, send.at[s], recvz.at[way, s, k], (h * Z + z_at(dz), mp)
            )
            thin = [hs for hs in (0, 1) if (s, way, hs) in THIN]
            if not thin:
                send_z().start()
            else:
                keep = k // 2 == h
                if len(thin) == 1:
                    keep = jnp.logical_or(keep, lax.rem(k, 2) != thin[0])

                @pl.when(keep)
                def _():
                    send_z().start()

    def over_y(s, own=False):
        if not own:
            await_recv(recv1.at[s, home])
        ref = land.at[dp, origin(s, yl)]
        piece_copy(ref, ref, send.at[s], recv1.at[s, home], ((1 - h) * Z + z, mp)).start()
        spread(s, home)

    def beside_y(s, own=False):
        if not own:
            await_recv(recvr.at[s])
        ref = staged.at[rank_at(1 - yl, x, c)] if own else relay.at[s]
        for hh in (0, 1):
            dev = (lax.rem(h + hh, 2) * Z + z, rank_at(1 - yl, x, c))
            piece_copy(ref, land.at[dp, origin(s, yl)], send.at[s], recv1.at[s, home], dev).start()

    def along_y(s):
        over_y(s)
        beside_y(s)

    def spread_rest(s):
        for k in (yl * 2 + 1 - h, (1 - yl) * 2 + h, (1 - yl) * 2 + 1 - h):
            await_recv(recv1.at[s, k])
            spread(s, k)

    def arrived(way, s, k):
        block = z_at(2) if way == 2 else (z_at(3) if way == 0 else z_at(1))
        return land.at[lax.rem(k, 2) * Z + block, origin(s, k // 2)]

    def onward(s):
        for row in (0, 1) if s in PLAIN else (0,):
            for way, dz in ((0, 1), (1, 3)):
                k = lax.rem(h + row, 2) * 2 + way
                await_recv(recvz.at[way, s, k])
                ref = arrived(way, s, k)
                piece_copy(ref, ref, send.at[s], recvz.at[2, s, k], (h * Z + z_at(dz), mp)).start()
        for way in (0, 1):
            for hs in (way, 1 - way):
                if (s, way, hs) in THIN:
                    if hs != way:
                        await_recv(recvz.at[way, s, h * 2 + hs])
                    over(way, s, h * 2 + hs)

    def over(way, s, k):
        ref = arrived(way, s, k)
        piece_copy(ref, ref, send.at[s], recvz.at[way, s, k], ((1 - h) * Z + z, mp)).start()

    def cross(s):
        if s in PLAIN:
            return
        for hs in (0, 1):
            await_recv(recvz.at[2, s, h * 2 + hs])
            over(2, s, h * 2 + hs)

    pltpu.make_async_copy(rank_hbm, rank_ref, rank_sem).wait()
    pltpu.make_async_copy(w, w, w_sem).wait()
    quantize(mp)
    land[dp, mp, :, :] = staged[mp, :, :]
    pl.semaphore_wait(barrier, N_MP + N_DP - 1)
    over_y(0, own=True)
    quantize(target(0, 1 - yl, c))
    beside_y(0, own=True)
    quantize(target(0, yl, 1 - c))
    quantize(target(0, 1 - yl, 1 - c))
    along_x(0, (1,))

    def rest(m, _):
        quantize_step(m)
        along_x(m, (0, 1))
        return 0

    lax.fori_loop(1, 2, rest, 0)
    along_y(1)
    spread_rest(0)
    lax.fori_loop(2, 4, rest, 0)

    parts[dp, :, :] = part[...]

    def give(n, _):
        dev = (lax.rem(dp + n, N_DP), mp)
        piece_copy(part, parts.at[dp], send_s, sem_a, dev).start()
        return 0

    lax.fori_loop(1, N_DP, give, 0)

    steps = {"Y": along_y, "R": spread_rest, "O": onward, "C": cross}
    for name, step in EARLY:
        steps[name](step)

    pltpu.make_async_copy(parts.at[pl.ds(0, 7)], parts.at[pl.ds(0, 7)], sem_a).wait()
    whole = jnp.sum(jnp.sum(parts[...], axis=0), axis=1, keepdims=True)
    sums[mp, :, :] = jnp.broadcast_to(whole, (N_MP, BLOCK))

    def share(n, _):
        dev = (dp, lax.rem(mp + n, N_MP))
        piece_copy(sums.at[mp], sums.at[mp], send_s, sem_b, dev).start()
        return 0

    lax.fori_loop(1, N_MP, share, 0)
    for name, step in LATE:
        steps[name](step)
    def sent(sem, n, ref):
        def one(_, carry):
            piece_copy(ref, ref, sem, w_sem, (dp, mp)).wait_send()
            return carry

        lax.fori_loop(0, n, one, 0)

    sent(send_x, 14, staged.at[0])
    sent(send_s, 7 + 15, part)
    for step in range(STEPS):
        sent(send.at[step], 15, staged.at[0])
    for step in range(STEPS):
        for way in (0, 1):
            if (step, way, 1 - way) not in THIN:
                await_recv(recvz.at[way, step, h * 2 + 1 - way])
            if step not in PLAIN:
                await_recv(recvz.at[way, step, (1 - h) * 2 + way])
            else:
                await_recv(recvz.at[2, step, h * 2 + way])
            await_recv(recvz.at[way, step, (1 - h) * 2 + 1 - way])
            await_recv(recvz.at[2, step, (1 - h) * 2 + way])
    pltpu.make_async_copy(sums.at[pl.ds(0, 15)], sums.at[pl.ds(0, 15)], sem_b).wait()


def settle(rank_hbm, land, sums, quant_out, scale_hbm, check_hbm, rank_ref, scale_out, check_out, rank_sem, sem, sem_s):
    pltpu.make_async_copy(rank_hbm, rank_ref, rank_sem).start()
    for d in range(N_DP):
        for i in range(N_MP):
            pltpu.make_async_copy(
                land.at[d, i, pl.ds(0, ROWS), :],
                quant_out.at[pl.ds(d * ROWS, ROWS), pl.ds(i * BLOCK, BLOCK)],
                sem,
            ).start()
    n = PIECE - ROWS
    k_rows = ROWS // BLOCK
    out_i = lax.broadcasted_iota(jnp.int32, (k_rows * N_MP, N_MP * n), 0)
    in_i = lax.broadcasted_iota(jnp.int32, (k_rows * N_MP, N_MP * n), 1)
    pick = (in_i == lax.rem(out_i, N_MP) * n + out_i // N_MP).astype(jnp.bfloat16)

    for d in range(N_DP):
        rows = land[d, :, pl.ds(ROWS, n), :].reshape(N_MP * n, BLOCK)
        ordered = jnp.dot(pick, rows, preferred_element_type=jnp.float32).astype(jnp.bfloat16)
        for k in range(k_rows):
            scale_out[:, pl.ds(d * ROWS + k * BLOCK, BLOCK)] = ordered[k * N_MP : (k + 1) * N_MP]

    pltpu.make_async_copy(rank_hbm, rank_ref, rank_sem).wait()
    row = lax.broadcasted_iota(jnp.int32, (N_MP, BLOCK), 0)
    lane = lax.broadcasted_iota(jnp.int32, (N_MP, BLOCK), 1)
    total = jnp.zeros((N_MP, BLOCK), jnp.float32)
    for j in range(N_MP):
        total = total + jnp.where(lane == lax.rem(row, 8) * N_MP + j, sums[:, rank_ref[j], :], 0.0)
    total = total / (127.0 * math.sqrt(D * BLOCK))
    for p in (0, 1):
        check_out[pl.ds(p, 1), :] = jnp.sum(total[p * 8 : (p + 1) * 8], axis=0, keepdims=True)

    small = (pltpu.make_async_copy(scale_out, scale_hbm, sem_s), pltpu.make_async_copy(check_out, check_hbm, rank_sem))
    for copy in small:
        copy.start()

    def done(n, _):
        pltpu.make_async_copy(
            land.at[0, 0, pl.ds(0, ROWS), :], quant_out.at[pl.ds(0, ROWS), pl.ds(0, BLOCK)], sem
        ).wait()
        return 0

    lax.fori_loop(0, N_DP * N_MP, done, 0)
    for copy in small:
        copy.wait()


def local(weight, rank_map):
    vmem = pl.BlockSpec(memory_space=pltpu.VMEM)
    hbm = pl.BlockSpec(memory_space=pltpu.HBM)
    rank_map = pltpu.with_memory_space_constraint(rank_map, pltpu.HBM)
    weight = pltpu.with_memory_space_constraint(weight, pltpu.HBM)
    dma = pltpu.SemaphoreType.DMA
    land, sums = pl.pallas_call(
        exchange,
        out_shape=(
            pltpu.VMEM((N_DP, N_MP, PIECE, BLOCK), jnp.bfloat16),
            pltpu.VMEM((N_MP, N_MP, BLOCK), jnp.float32),
        ),
        in_specs=[hbm, hbm],
        out_specs=(vmem, vmem),
        scratch_shapes=[
            pltpu.SMEM((N_MP,), jnp.int32),
            pltpu.VMEM((N_MP, ROWS, BLOCK), jnp.bfloat16),
            pltpu.VMEM((N_MP, PIECE, BLOCK), jnp.bfloat16),
            pltpu.VMEM((STEPS, PIECE, BLOCK), jnp.bfloat16),
            pltpu.VMEM((N_MP, BLOCK), jnp.float32),
            pltpu.VMEM((N_DP, N_MP, BLOCK), jnp.float32),
            dma(()),
            dma(()),
            dma((STEPS, 4)),
            dma((STEPS,)),
            dma((3, STEPS, 4)),
            dma((STEPS,)),
            dma(()),
            dma(()),
            dma(()),
            dma(()),
        ],
        compiler_params=pltpu.CompilerParams(collective_id=0, has_side_effects=True, vmem_limit_bytes=12 * MIB),
        name="exchange",
    )(rank_map, weight)
    quant_out, scale_out, check = pl.pallas_call(
        settle,
        out_shape=(
            pltpu.HBM((D, N_MP * BLOCK), jnp.bfloat16),
            pltpu.HBM((N_MP, D), jnp.bfloat16),
            pltpu.HBM((2, BLOCK), jnp.float32),
        ),
        in_specs=[hbm, vmem, vmem],
        out_specs=(hbm, hbm, hbm),
        scratch_shapes=[
            pltpu.SMEM((N_MP,), jnp.int32),
            pltpu.VMEM((N_MP, D), jnp.bfloat16),
            pltpu.VMEM((2, BLOCK), jnp.float32),
            dma(()),
            dma(()),
            dma(()),
        ],
        compiler_params=pltpu.CompilerParams(vmem_limit_bytes=12 * MIB),
        name="settle",
    )(rank_map, land, sums)
    return quant_out, scale_out.T, check.reshape(2 * BLOCK)


def solution(mesh):
    return jax.shard_map(
        local,
        mesh=mesh,
        in_specs=(P("dp", "mp"), P()),
        out_specs=(P(None, "mp"), P(None, "mp"), P()),
        check_vma=False,
    )
```

```python
import functools
import math

import jax
import jax.numpy as jnp
from jax import lax
from jax.experimental import pallas as pl
from jax.experimental.pallas import tpu as pltpu
from jax.sharding import PartitionSpec as P

MESH = pl.DeviceIdType.MESH
D = 5120
floor_ratio = 0.25
BLOCK = 128
ROWS = 640
PIECE = 648
N_MP = 16
N_DP = 8
STEPS = 8
Z = 4
MIB = 1024 * 1024
THIN = (
    (1, 0, 0),
    (1, 0, 1),
    (2, 1, 0),
    (2, 1, 1),
    (3, 0, 0),
    (3, 0, 1),
    (4, 1, 0),
)
HALF = ((4, 1, 1), )
CUT = 328
PLAIN = (7,)
EARLY = (
    ("Y", 2),
    ("R", 1),
    ("Y", 3),
    ("O", 0),
    ("Y", 4),
    ("R", 2),
    ("O", 1),
    ("C", 0),
    ("Y", 5),
    ("R", 3),
    ("O", 2),
    ("C", 1),
    ("Y", 6),
    ("R", 4),
    ("O", 3),
    ("C", 2),
    ("Y", 7),
    ("R", 5),
    ("O", 4),
    ("C", 3),
    ("R", 6),
    ("O", 5),
    ("C", 4),
    ("O", 6),
    ("C", 5),
    ("R", 7),
)
LATE = (
    ("C", 6),
    ("O", 7),
)


def exchange(
    rank_hbm, w_hbm, land, sums, rank_ref, w, staged, relay, part, parts, rank_sem, w_sem, recv1, recvr, recvz, send, send_x, sem_a, sem_b, send_s
):
    dp = lax.axis_index("dp")
    mp = lax.axis_index("mp")
    h, z = dp // Z, lax.rem(dp, Z)
    yl, x, c = mp // 8, lax.rem(mp // 2, 4), lax.rem(mp, 2)
    home = yl * 2 + h

    pltpu.make_async_copy(rank_hbm, rank_ref, rank_sem).start()
    for q in range(N_MP):
        pltpu.make_async_copy(w_hbm.at[:, pl.ds(q * BLOCK, BLOCK)], w.at[q], w_sem).start()

    def z_at(dz):
        return lax.rem(z + dz, Z)

    def rank_at(yy, xx, cc):
        return yy * 8 + xx * 2 + cc

    def shift(m):
        return m + m // 2 - 2 * (m // 3)

    def target(m, yy, cc):
        return rank_at(yy, lax.rem(x + shift(m), 4), cc)

    def origin(s, yy):
        return rank_at(yy, lax.rem(x + 4 - shift(s // 2), 4), lax.rem(c + s, 2))

    barrier = pltpu.get_barrier_semaphore()

    def greet(dev):
        pl.semaphore_signal(barrier, inc=1, device_id=dev, device_id_type=MESH)

    def greet_mp(n, _):
        greet((dp, lax.rem(mp + n, N_MP)))
        return 0

    def greet_dp(n, _):
        greet((lax.rem(dp + n, N_DP), mp))
        return 0

    lax.fori_loop(1, N_MP, greet_mp, 0)
    lax.fori_loop(1, N_DP, greet_dp, 0)
    greet(((1 - h) * Z + z, rank_at(1 - yl, x, c)))

    rows_i = lax.broadcasted_iota(jnp.int32, (BLOCK, BLOCK), 0)
    cols_i = lax.broadcasted_iota(jnp.int32, (BLOCK, BLOCK), 1)
    diag = rows_i == cols_i

    def quantize(r):
        j = jnp.int32(0)
        for q in range(N_MP):
            j = j + jnp.where(rank_ref[q] == r, jnp.int32(q), jnp.int32(0))
        j = jnp.minimum(j, N_MP - 1)
        acc = jnp.zeros((8, BLOCK), jnp.float32)
        scales = []
        for k in range(ROWS // BLOCK):
            blk = w[j, pl.ds(k * BLOCK, BLOCK), :].astype(jnp.float32)
            peak = jnp.max(jnp.abs(blk), axis=1, keepdims=True)
            scale = (jnp.maximum(peak, floor_ratio / math.sqrt(D)) / 127.0).astype(jnp.bfloat16).astype(jnp.float32)
            scale = jnp.broadcast_to(scale, (BLOCK, BLOCK))
            quant = (blk / scale).astype(jnp.bfloat16)
            staged[r, pl.ds(k * BLOCK, BLOCK), :] = quant
            acc = acc + jnp.sum(quant.astype(jnp.float32).reshape(BLOCK // 8, 8, BLOCK), axis=0)
            scales.append(jnp.sum(jnp.where(diag, scale, 0.0), axis=0, keepdims=True))
        scales.append(jnp.zeros((PIECE - ROWS - len(scales), BLOCK), jnp.float32))
        staged[r, pl.ds(ROWS, PIECE - ROWS), :] = jnp.concatenate(scales, axis=0).astype(jnp.bfloat16)
        part[pl.ds(r, 1), :] = jnp.sum(acc, axis=0, keepdims=True)

    def quantize_step(m):
        def one(n, _):
            quantize(target(m, n // 2, lax.rem(n, 2)))
            return 0

        lax.fori_loop(0, 4, one, 0)

    def piece_copy(src, dst, sem_s, sem_r, dev):
        return pltpu.make_async_remote_copy(src, dst, sem_s, sem_r, device_id=dev, device_id_type=MESH)

    def await_recv(sem):
        piece_copy(staged.at[0], staged.at[0], send_x, sem, (dp, mp)).wait_recv()

    def along_x(m, cores):
        for cc in cores:
            to = lax.rem(c + cc, 2)
            s = 2 * m + cc
            dev = (dp, target(m, yl, to))
            piece_copy(staged.at[target(m, yl, to)], land.at[dp, mp], send_x, recv1.at[s, home], dev).start()
            piece_copy(staged.at[target(m, 1 - yl, to)], relay.at[s], send_x, recvr.at[s], dev).start()

    def spread(s, k):
        ref = land.at[lax.rem(k, 2) * Z + z, origin(s, k // 2)]
        for way, dz in ((0, 1), (1, 3)):
            send_z = functools.partial(
                piece_copy, ref, ref, send.at[s], recvz.at[way, s, k], (h * Z + z_at(dz), mp)
            )
            thin = [hs for hs in (0, 1) if (s, way, hs) in THIN]
            half = [hs for hs in (0, 1) if (s, way, hs) in HALF]
            if half:
                whole = jnp.logical_or(k // 2 == h, lax.rem(k, 2) != half[0])

                full = whole
                if thin:
                    full = jnp.logical_or(k // 2 == h, jnp.logical_and(whole, lax.rem(k, 2) != thin[0]))

                @pl.when(full)
                def _():
                    send_z().start()

                @pl.when(jnp.logical_not(whole))
                def _():
                    top = ref.at[pl.ds(0, CUT), :]
                    piece_copy(top, top, send.at[s], recvz.at[way, s, k], (h * Z + z_at(dz), mp)).start()

            elif not thin:
                send_z().start()
            else:
                keep = k // 2 == h
                if len(thin) == 1:
                    keep = jnp.logical_or(keep, lax.rem(k, 2) != thin[0])

                @pl.when(keep)
                def _():
                    send_z().start()

    def over_y(s, own=False):
        if not own:
            await_recv(recv1.at[s, home])
        ref = land.at[dp, origin(s, yl)]
        spread(s, home)
        piece_copy(ref, ref, send.at[s], recv1.at[s, home], ((1 - h) * Z + z, mp)).start()

    def beside_y(s, own=False):
        if not own:
            await_recv(recvr.at[s])
        ref = staged.at[rank_at(1 - yl, x, c)] if own else relay.at[s]
        for hh in (0, 1):
            dev = (lax.rem(h + hh, 2) * Z + z, rank_at(1 - yl, x, c))
            piece_copy(ref, land.at[dp, origin(s, yl)], send.at[s], recv1.at[s, home], dev).start()

    def along_y(s):
        over_y(s)
        beside_y(s)

    def spread_rest(s):
        for k in (yl * 2 + 1 - h, (1 - yl) * 2 + h, (1 - yl) * 2 + 1 - h):
            await_recv(recv1.at[s, k])
            spread(s, k)

    def arrived(way, s, k):
        block = z_at(2) if way == 2 else (z_at(3) if way == 0 else z_at(1))
        return land.at[lax.rem(k, 2) * Z + block, origin(s, k // 2)]

    def onward(s):
        for row in (0, 1) if s in PLAIN else (0,):
            for way, dz in ((0, 1), (1, 3)):
                k = lax.rem(h + row, 2) * 2 + way
                await_recv(recvz.at[way, s, k])
                ref = arrived(way, s, k)
                piece_copy(ref, ref, send.at[s], recvz.at[2, s, k], (h * Z + z_at(dz), mp)).start()
        for way in (0, 1):
            for hs in (way, 1 - way):
                if (s, way, hs) in THIN or (s, way, hs) in HALF:
                    if hs != way:
                        await_recv(recvz.at[way, s, h * 2 + hs])
                    over(way, s, h * 2 + hs, (s, way, hs) in HALF)

    def over(way, s, k, rest=False):
        ref = arrived(way, s, k)
        if rest:
            ref = ref.at[pl.ds(CUT, PIECE - CUT), :]
        piece_copy(ref, ref, send.at[s], recvz.at[way, s, k], ((1 - h) * Z + z, mp)).start()

    def cross(s):
        if s in PLAIN:
            return
        for hs in (0, 1):
            await_recv(recvz.at[2, s, h * 2 + hs])
            over(2, s, h * 2 + hs)

    pltpu.make_async_copy(rank_hbm, rank_ref, rank_sem).wait()
    pltpu.make_async_copy(w, w, w_sem).wait()
    quantize(mp)
    land[dp, mp, :, :] = staged[mp, :, :]
    pl.semaphore_wait(barrier, N_MP + N_DP - 1)
    over_y(0, own=True)
    quantize(target(0, 1 - yl, c))
    beside_y(0, own=True)
    quantize(target(0, yl, 1 - c))
    quantize(target(0, 1 - yl, 1 - c))
    along_x(0, (1,))

    def rest(m, _):
        quantize_step(m)
        along_x(m, (0, 1))
        return 0

    lax.fori_loop(1, 2, rest, 0)
    along_y(1)
    spread_rest(0)
    lax.fori_loop(2, 4, rest, 0)

    parts[dp, :, :] = part[...]

    def give(n, _):
        dev = (lax.rem(dp + n, N_DP), mp)
        piece_copy(part, parts.at[dp], send_s, sem_a, dev).start()
        return 0

    lax.fori_loop(1, N_DP, give, 0)

    steps = {"Y": along_y, "R": spread_rest, "O": onward, "C": cross}
    for name, step in EARLY:
        steps[name](step)

    pltpu.make_async_copy(parts.at[pl.ds(0, 7)], parts.at[pl.ds(0, 7)], sem_a).wait()
    whole = jnp.sum(jnp.sum(parts[...], axis=0), axis=1, keepdims=True)
    sums[mp, :, :] = jnp.broadcast_to(whole, (N_MP, BLOCK))

    def share(n, _):
        dev = (dp, lax.rem(mp + n, N_MP))
        piece_copy(sums.at[mp], sums.at[mp], send_s, sem_b, dev).start()
        return 0

    lax.fori_loop(1, N_MP, share, 0)
    for name, step in LATE:
        steps[name](step)
    def sent(sem, n, ref):
        def one(_, carry):
            piece_copy(ref, ref, sem, w_sem, (dp, mp)).wait_send()
            return carry

        lax.fori_loop(0, n, one, 0)

    sent(send_x, 14, staged.at[0])
    sent(send_s, 7 + 15, part)
    for step in range(STEPS):
        sent(send.at[step], 15, staged.at[0])
    for step in range(STEPS):
        for way in (0, 1):
            if (step, way, 1 - way) not in THIN + HALF:
                await_recv(recvz.at[way, step, h * 2 + 1 - way])
            if step not in PLAIN:
                await_recv(recvz.at[way, step, (1 - h) * 2 + way])
            else:
                await_recv(recvz.at[2, step, h * 2 + way])
            await_recv(recvz.at[way, step, (1 - h) * 2 + 1 - way])
            await_recv(recvz.at[2, step, (1 - h) * 2 + way])
    pltpu.make_async_copy(sums.at[pl.ds(0, 15)], sums.at[pl.ds(0, 15)], sem_b).wait()


def settle(rank_hbm, land, sums, quant_out, scale_hbm, check_hbm, rank_ref, scale_out, check_out, rank_sem, sem, sem_s):
    pltpu.make_async_copy(rank_hbm, rank_ref, rank_sem).start()
    for d in range(N_DP):
        for i in range(N_MP):
            pltpu.make_async_copy(
                land.at[d, i, pl.ds(0, ROWS), :],
                quant_out.at[pl.ds(d * ROWS, ROWS), pl.ds(i * BLOCK, BLOCK)],
                sem,
            ).start()
    n = PIECE - ROWS
    k_rows = ROWS // BLOCK
    out_i = lax.broadcasted_iota(jnp.int32, (k_rows * N_MP, N_MP * n), 0)
    in_i = lax.broadcasted_iota(jnp.int32, (k_rows * N_MP, N_MP * n), 1)
    pick = (in_i == lax.rem(out_i, N_MP) * n + out_i // N_MP).astype(jnp.bfloat16)

    for d in range(N_DP):
        rows = land[d, :, pl.ds(ROWS, n), :].reshape(N_MP * n, BLOCK)
        ordered = jnp.dot(pick, rows, preferred_element_type=jnp.float32).astype(jnp.bfloat16)
        for k in range(k_rows):
            scale_out[:, pl.ds(d * ROWS + k * BLOCK, BLOCK)] = ordered[k * N_MP : (k + 1) * N_MP]

    pltpu.make_async_copy(rank_hbm, rank_ref, rank_sem).wait()
    row = lax.broadcasted_iota(jnp.int32, (N_MP, BLOCK), 0)
    lane = lax.broadcasted_iota(jnp.int32, (N_MP, BLOCK), 1)
    total = jnp.zeros((N_MP, BLOCK), jnp.float32)
    for j in range(N_MP):
        total = total + jnp.where(lane == lax.rem(row, 8) * N_MP + j, sums[:, rank_ref[j], :], 0.0)
    total = total / (127.0 * math.sqrt(D * BLOCK))
    for p in (0, 1):
        check_out[pl.ds(p, 1), :] = jnp.sum(total[p * 8 : (p + 1) * 8], axis=0, keepdims=True)

    small = (pltpu.make_async_copy(scale_out, scale_hbm, sem_s), pltpu.make_async_copy(check_out, check_hbm, rank_sem))
    for copy in small:
        copy.start()

    def done(n, _):
        pltpu.make_async_copy(
            land.at[0, 0, pl.ds(0, ROWS), :], quant_out.at[pl.ds(0, ROWS), pl.ds(0, BLOCK)], sem
        ).wait()
        return 0

    lax.fori_loop(0, N_DP * N_MP, done, 0)
    for copy in small:
        copy.wait()


def local(weight, rank_map):
    vmem = pl.BlockSpec(memory_space=pltpu.VMEM)
    hbm = pl.BlockSpec(memory_space=pltpu.HBM)
    rank_map = pltpu.with_memory_space_constraint(rank_map, pltpu.HBM)
    weight = pltpu.with_memory_space_constraint(weight, pltpu.HBM)
    dma = pltpu.SemaphoreType.DMA
    land, sums = pl.pallas_call(
        exchange,
        out_shape=(
            pltpu.VMEM((N_DP, N_MP, PIECE, BLOCK), jnp.bfloat16),
            pltpu.VMEM((N_MP, N_MP, BLOCK), jnp.float32),
        ),
        in_specs=[hbm, hbm],
        out_specs=(vmem, vmem),
        scratch_shapes=[
            pltpu.SMEM((N_MP,), jnp.int32),
            pltpu.VMEM((N_MP, ROWS, BLOCK), jnp.bfloat16),
            pltpu.VMEM((N_MP, PIECE, BLOCK), jnp.bfloat16),
            pltpu.VMEM((STEPS, PIECE, BLOCK), jnp.bfloat16),
            pltpu.VMEM((N_MP, BLOCK), jnp.float32),
            pltpu.VMEM((N_DP, N_MP, BLOCK), jnp.float32),
            dma(()),
            dma(()),
            dma((STEPS, 4)),
            dma((STEPS,)),
            dma((3, STEPS, 4)),
            dma((STEPS,)),
            dma(()),
            dma(()),
            dma(()),
            dma(()),
        ],
        compiler_params=pltpu.CompilerParams(collective_id=0, has_side_effects=True, vmem_limit_bytes=12 * MIB),
        name="exchange",
    )(rank_map, weight)
    quant_out, scale_out, check = pl.pallas_call(
        settle,
        out_shape=(
            pltpu.HBM((D, N_MP * BLOCK), jnp.bfloat16),
            pltpu.HBM((N_MP, D), jnp.bfloat16),
            pltpu.HBM((2, BLOCK), jnp.float32),
        ),
        in_specs=[hbm, vmem, vmem],
        out_specs=(hbm, hbm, hbm),
        scratch_shapes=[
            pltpu.SMEM((N_MP,), jnp.int32),
            pltpu.VMEM((N_MP, D), jnp.bfloat16),
            pltpu.VMEM((2, BLOCK), jnp.float32),
            dma(()),
            dma(()),
            dma(()),
        ],
        compiler_params=pltpu.CompilerParams(vmem_limit_bytes=12 * MIB),
        name="settle",
    )(rank_map, land, sums)
    return quant_out, scale_out.T, check.reshape(2 * BLOCK)


def solution(mesh):
    return jax.shard_map(
        local,
        mesh=mesh,
        in_specs=(P("dp", "mp"), P()),
        out_specs=(P(None, "mp"), P(None, "mp"), P()),
        check_vma=False,
    )
```

```python
import functools
import math

import jax
import jax.numpy as jnp
from jax import lax
from jax.experimental import pallas as pl
from jax.experimental.pallas import tpu as pltpu
from jax.sharding import PartitionSpec as P

MESH = pl.DeviceIdType.MESH
D = 5120
floor_ratio = 0.25
BLOCK = 128
ROWS = 640
PIECE = 648
N_MP = 16
N_DP = 8
STEPS = 8
Z = 4
MIB = 1024 * 1024
THIN = (
    (1, 0, 0),
    (1, 0, 1),
    (2, 1, 0),
    (2, 1, 1),
    (3, 0, 0),
    (3, 0, 1),
    (4, 1, 0),
)
PLAIN = (7,)
EARLY = (
    ("Y", 2),
    ("R", 1),
    ("Y", 3),
    ("O", 0),
    ("Y", 4),
    ("R", 2),
    ("O", 1),
    ("C", 0),
    ("Y", 5),
    ("R", 3),
    ("O", 2),
    ("C", 1),
    ("Y", 6),
    ("R", 4),
    ("O", 3),
    ("C", 2),
    ("Y", 7),
)
LATE = (
    ("R", 5),
    ("O", 4),
    ("C", 3),
    ("R", 6),
    ("O", 5),
    ("C", 4),
    ("O", 6),
    ("C", 5),
    ("R", 7),
    ("C", 6),
    ("O", 7),
)


def exchange(
    rank_hbm, w_hbm, land, sums, rank_ref, w, staged, relay, part, parts, rank_sem, w_sem, recv1, recvr, recvz, send, send_x, sem_a, sem_b, send_s
):
    dp = lax.axis_index("dp")
    mp = lax.axis_index("mp")
    h, z = dp // Z, lax.rem(dp, Z)
    yl, x, c = mp // 8, lax.rem(mp // 2, 4), lax.rem(mp, 2)
    home = yl * 2 + h

    pltpu.make_async_copy(rank_hbm, rank_ref, rank_sem).start()
    for q in range(N_MP):
        pltpu.make_async_copy(w_hbm.at[:, pl.ds(q * BLOCK, BLOCK)], w.at[q], w_sem).start()

    def z_at(dz):
        return lax.rem(z + dz, Z)

    def rank_at(yy, xx, cc):
        return yy * 8 + xx * 2 + cc

    def shift(m):
        return m + m // 2 - 2 * (m // 3)

    def target(m, yy, cc):
        return rank_at(yy, lax.rem(x + shift(m), 4), cc)

    def origin(s, yy):
        return rank_at(yy, lax.rem(x + 4 - shift(s // 2), 4), lax.rem(c + s, 2))

    barrier = pltpu.get_barrier_semaphore()

    def greet(dev):
        pl.semaphore_signal(barrier, inc=1, device_id=dev, device_id_type=MESH)

    def greet_mp(n, _):
        greet((dp, lax.rem(mp + n, N_MP)))
        return 0

    def greet_dp(n, _):
        greet((lax.rem(dp + n, N_DP), mp))
        return 0

    lax.fori_loop(1, N_MP, greet_mp, 0)
    lax.fori_loop(1, N_DP, greet_dp, 0)
    greet(((1 - h) * Z + z, rank_at(1 - yl, x, c)))

    rows_i = lax.broadcasted_iota(jnp.int32, (BLOCK, BLOCK), 0)
    cols_i = lax.broadcasted_iota(jnp.int32, (BLOCK, BLOCK), 1)
    diag = rows_i == cols_i

    def quantize(r):
        j = jnp.int32(0)
        for q in range(N_MP):
            j = j + jnp.where(rank_ref[q] == r, jnp.int32(q), jnp.int32(0))
        j = jnp.minimum(j, N_MP - 1)
        acc = jnp.zeros((8, BLOCK), jnp.float32)
        scales = []
        for k in range(ROWS // BLOCK):
            blk = w[j, pl.ds(k * BLOCK, BLOCK), :].astype(jnp.float32)
            peak = jnp.max(jnp.abs(blk), axis=1, keepdims=True)
            scale = (jnp.maximum(peak, floor_ratio / math.sqrt(D)) / 127.0).astype(jnp.bfloat16).astype(jnp.float32)
            scale = jnp.broadcast_to(scale, (BLOCK, BLOCK))
            quant = (blk / scale).astype(jnp.bfloat16)
            staged[r, pl.ds(k * BLOCK, BLOCK), :] = quant
            acc = acc + jnp.sum(quant.astype(jnp.float32).reshape(BLOCK // 8, 8, BLOCK), axis=0)
            scales.append(jnp.sum(jnp.where(diag, scale, 0.0), axis=0, keepdims=True))
        scales.append(jnp.zeros((PIECE - ROWS - len(scales), BLOCK), jnp.float32))
        staged[r, pl.ds(ROWS, PIECE - ROWS), :] = jnp.concatenate(scales, axis=0).astype(jnp.bfloat16)
        part[pl.ds(r, 1), :] = jnp.sum(acc, axis=0, keepdims=True)

    def quantize_step(m):
        def one(n, _):
            quantize(target(m, n // 2, lax.rem(n, 2)))
            return 0

        lax.fori_loop(0, 4, one, 0)

    def piece_copy(src, dst, sem_s, sem_r, dev):
        return pltpu.make_async_remote_copy(src, dst, sem_s, sem_r, device_id=dev, device_id_type=MESH)

    def await_recv(sem):
        piece_copy(staged.at[0], staged.at[0], send_x, sem, (dp, mp)).wait_recv()

    def along_x(m, cores):
        for cc in cores:
            to = lax.rem(c + cc, 2)
            s = 2 * m + cc
            dev = (dp, target(m, yl, to))
            piece_copy(staged.at[target(m, yl, to)], land.at[dp, mp], send_x, recv1.at[s, home], dev).start()
            piece_copy(staged.at[target(m, 1 - yl, to)], relay.at[s], send_x, recvr.at[s], dev).start()

    def spread(s, k):
        ref = land.at[lax.rem(k, 2) * Z + z, origin(s, k // 2)]
        for way, dz in ((0, 1), (1, 3)):
            send_z = functools.partial(
                piece_copy, ref, ref, send.at[s], recvz.at[way, s, k], (h * Z + z_at(dz), mp)
            )
            thin = [hs for hs in (0, 1) if (s, way, hs) in THIN]
            if not thin:
                send_z().start()
            else:
                keep = k // 2 == h
                if len(thin) == 1:
                    keep = jnp.logical_or(keep, lax.rem(k, 2) != thin[0])

                @pl.when(keep)
                def _():
                    send_z().start()

    def over_y(s, own=False):
        if not own:
            await_recv(recv1.at[s, home])
        ref = land.at[dp, origin(s, yl)]
        piece_copy(ref, ref, send.at[s], recv1.at[s, home], ((1 - h) * Z + z, mp)).start()
        spread(s, home)

    def beside_y(s, own=False):
        if not own:
            await_recv(recvr.at[s])
        ref = staged.at[rank_at(1 - yl, x, c)] if own else relay.at[s]
        for hh in (0, 1):
            dev = (lax.rem(h + hh, 2) * Z + z, rank_at(1 - yl, x, c))
            piece_copy(ref, land.at[dp, origin(s, yl)], send.at[s], recv1.at[s, home], dev).start()

    def along_y(s):
        over_y(s)
        beside_y(s)

    def spread_rest(s):
        for k in (yl * 2 + 1 - h, (1 - yl) * 2 + h, (1 - yl) * 2 + 1 - h):
            await_recv(recv1.at[s, k])
            spread(s, k)

    def arrived(way, s, k):
        block = z_at(2) if way == 2 else (z_at(3) if way == 0 else z_at(1))
        return land.at[lax.rem(k, 2) * Z + block, origin(s, k // 2)]

    def onward(s):
        for row in (0, 1) if s in PLAIN else (0,):
            for way, dz in ((0, 1), (1, 3)):
                k = lax.rem(h + row, 2) * 2 + way
                await_recv(recvz.at[way, s, k])
                ref = arrived(way, s, k)
                piece_copy(ref, ref, send.at[s], recvz.at[2, s, k], (h * Z + z_at(dz), mp)).start()
        for way in (0, 1):
            for hs in (way, 1 - way):
                if (s, way, hs) in THIN:
                    if hs != way:
                        await_recv(recvz.at[way, s, h * 2 + hs])
                    over(way, s, h * 2 + hs)

    def over(way, s, k):
        ref = arrived(way, s, k)
        piece_copy(ref, ref, send.at[s], recvz.at[way, s, k], ((1 - h) * Z + z, mp)).start()

    def cross(s):
        if s in PLAIN:
            return
        for hs in (0, 1):
            await_recv(recvz.at[2, s, h * 2 + hs])
            over(2, s, h * 2 + hs)

    pltpu.make_async_copy(rank_hbm, rank_ref, rank_sem).wait()
    pltpu.make_async_copy(w, w, w_sem).wait()
    quantize(mp)
    land[dp, mp, :, :] = staged[mp, :, :]
    pl.semaphore_wait(barrier, N_MP + N_DP - 1)
    over_y(0, own=True)
    quantize(target(0, 1 - yl, c))
    beside_y(0, own=True)
    quantize(target(0, yl, 1 - c))
    quantize(target(0, 1 - yl, 1 - c))
    along_x(0, (1,))

    def rest(m, _):
        quantize_step(m)
        along_x(m, (0, 1))
        return 0

    lax.fori_loop(1, 2, rest, 0)
    along_y(1)
    spread_rest(0)
    lax.fori_loop(2, 4, rest, 0)

    parts[dp, :, :] = part[...]

    def give(n, _):
        dev = (lax.rem(dp + n, N_DP), mp)
        piece_copy(part, parts.at[dp], send_s, sem_a, dev).start()
        return 0

    lax.fori_loop(1, N_DP, give, 0)

    steps = {"Y": along_y, "R": spread_rest, "O": onward, "C": cross}
    for name, step in EARLY:
        steps[name](step)

    pltpu.make_async_copy(parts.at[pl.ds(0, 7)], parts.at[pl.ds(0, 7)], sem_a).wait()
    whole = jnp.sum(jnp.sum(parts[...], axis=0), axis=1, keepdims=True)
    sums[mp, :, :] = jnp.broadcast_to(whole, (N_MP, BLOCK))

    def share(n, _):
        dev = (dp, lax.rem(mp + n, N_MP))
        piece_copy(sums.at[mp], sums.at[mp], send_s, sem_b, dev).start()
        return 0

    lax.fori_loop(1, N_MP, share, 0)
    for name, step in LATE:
        steps[name](step)
    def sent(sem, n, ref):
        def one(_, carry):
            piece_copy(ref, ref, sem, w_sem, (dp, mp)).wait_send()
            return carry

        lax.fori_loop(0, n, one, 0)

    sent(send_x, 14, staged.at[0])
    sent(send_s, 7 + 15, part)
    for step in range(STEPS):
        sent(send.at[step], 15, staged.at[0])
    for step in range(STEPS):
        for way in (0, 1):
            if (step, way, 1 - way) not in THIN:
                await_recv(recvz.at[way, step, h * 2 + 1 - way])
            if step not in PLAIN:
                await_recv(recvz.at[way, step, (1 - h) * 2 + way])
            else:
                await_recv(recvz.at[2, step, h * 2 + way])
            await_recv(recvz.at[way, step, (1 - h) * 2 + 1 - way])
            await_recv(recvz.at[2, step, (1 - h) * 2 + way])
    pltpu.make_async_copy(sums.at[pl.ds(0, 15)], sums.at[pl.ds(0, 15)], sem_b).wait()


def settle(rank_hbm, land, sums, quant_out, scale_hbm, check_hbm, rank_ref, scale_out, check_out, rank_sem, sem, sem_s):
    pltpu.make_async_copy(rank_hbm, rank_ref, rank_sem).start()
    for d in range(N_DP):
        for i in range(N_MP):
            pltpu.make_async_copy(
                land.at[d, i, pl.ds(0, ROWS), :],
                quant_out.at[pl.ds(d * ROWS, ROWS), pl.ds(i * BLOCK, BLOCK)],
                sem,
            ).start()
    n = PIECE - ROWS
    k_rows = ROWS // BLOCK
    out_i = lax.broadcasted_iota(jnp.int32, (k_rows * N_MP, N_MP * n), 0)
    in_i = lax.broadcasted_iota(jnp.int32, (k_rows * N_MP, N_MP * n), 1)
    pick = (in_i == lax.rem(out_i, N_MP) * n + out_i // N_MP).astype(jnp.bfloat16)

    for d in range(N_DP):
        rows = land[d, :, pl.ds(ROWS, n), :].reshape(N_MP * n, BLOCK)
        ordered = jnp.dot(pick, rows, preferred_element_type=jnp.float32).astype(jnp.bfloat16)
        for k in range(k_rows):
            scale_out[:, pl.ds(d * ROWS + k * BLOCK, BLOCK)] = ordered[k * N_MP : (k + 1) * N_MP]

    pltpu.make_async_copy(rank_hbm, rank_ref, rank_sem).wait()
    row = lax.broadcasted_iota(jnp.int32, (N_MP, BLOCK), 0)
    lane = lax.broadcasted_iota(jnp.int32, (N_MP, BLOCK), 1)
    total = jnp.zeros((N_MP, BLOCK), jnp.float32)
    for j in range(N_MP):
        total = total + jnp.where(lane == lax.rem(row, 8) * N_MP + j, sums[:, rank_ref[j], :], 0.0)
    total = total / (127.0 * math.sqrt(D * BLOCK))
    for p in (0, 1):
        check_out[pl.ds(p, 1), :] = jnp.sum(total[p * 8 : (p + 1) * 8], axis=0, keepdims=True)

    small = (pltpu.make_async_copy(scale_out, scale_hbm, sem_s), pltpu.make_async_copy(check_out, check_hbm, rank_sem))
    for copy in small:
        copy.start()

    def done(n, _):
        pltpu.make_async_copy(
            land.at[0, 0, pl.ds(0, ROWS), :], quant_out.at[pl.ds(0, ROWS), pl.ds(0, BLOCK)], sem
        ).wait()
        return 0

    lax.fori_loop(0, N_DP * N_MP, done, 0)
    for copy in small:
        copy.wait()


def local(weight, rank_map):
    vmem = pl.BlockSpec(memory_space=pltpu.VMEM)
    hbm = pl.BlockSpec(memory_space=pltpu.HBM)
    rank_map = pltpu.with_memory_space_constraint(rank_map, pltpu.HBM)
    weight = pltpu.with_memory_space_constraint(weight, pltpu.HBM)
    dma = pltpu.SemaphoreType.DMA
    land, sums = pl.pallas_call(
        exchange,
        out_shape=(
            pltpu.VMEM((N_DP, N_MP, PIECE, BLOCK), jnp.bfloat16),
            pltpu.VMEM((N_MP, N_MP, BLOCK), jnp.float32),
        ),
        in_specs=[hbm, hbm],
        out_specs=(vmem, vmem),
        scratch_shapes=[
            pltpu.SMEM((N_MP,), jnp.int32),
            pltpu.VMEM((N_MP, ROWS, BLOCK), jnp.bfloat16),
            pltpu.VMEM((N_MP, PIECE, BLOCK), jnp.bfloat16),
            pltpu.VMEM((STEPS, PIECE, BLOCK), jnp.bfloat16),
            pltpu.VMEM((N_MP, BLOCK), jnp.float32),
            pltpu.VMEM((N_DP, N_MP, BLOCK), jnp.float32),
            dma(()),
            dma(()),
            dma((STEPS, 4)),
            dma((STEPS,)),
            dma((3, STEPS, 4)),
            dma((STEPS,)),
            dma(()),
            dma(()),
            dma(()),
            dma(()),
        ],
        compiler_params=pltpu.CompilerParams(collective_id=0, has_side_effects=True, vmem_limit_bytes=12 * MIB),
        name="exchange",
    )(rank_map, weight)
    quant_out, scale_out, check = pl.pallas_call(
        settle,
        out_shape=(
            pltpu.HBM((D, N_MP * BLOCK), jnp.bfloat16),
            pltpu.HBM((N_MP, D), jnp.bfloat16),
            pltpu.HBM((2, BLOCK), jnp.float32),
        ),
        in_specs=[hbm, vmem, vmem],
        out_specs=(hbm, hbm, hbm),
        scratch_shapes=[
            pltpu.SMEM((N_MP,), jnp.int32),
            pltpu.VMEM((N_MP, D), jnp.bfloat16),
            pltpu.VMEM((2, BLOCK), jnp.float32),
            dma(()),
            dma(()),
            dma(()),
        ],
        compiler_params=pltpu.CompilerParams(vmem_limit_bytes=12 * MIB),
        name="settle",
    )(rank_map, land, sums)
    return quant_out, scale_out.T, check.reshape(2 * BLOCK)


def solution(mesh):
    return jax.shard_map(
        local,
        mesh=mesh,
        in_specs=(P("dp", "mp"), P()),
        out_specs=(P(None, "mp"), P(None, "mp"), P()),
        check_vma=False,
    )
```
